32 devices in a mesh: row: 8 (over y, x, core), col: 4 (over z).
Axes of the slice: x: 2, y: 2, z: 4, core: 2. Of those that a mesh axis runs over, the one named last changes fastest.
Arguments:
- constraint_tiles: float32 [768, 4, 128, 128], P('row', 'col'), may hold values from -0.375 to 0.375
- constraint_rows: int32 [768, 4], P('row', 'col'), may hold values from 0 to 191
- constraint_cols: int32 [768, 4], P('row', 'col'), may hold values from 0 to 255
- factor_tiles: float32 [384, 4, 128, 128], P('row', 'col'), may hold values from -0.3125 to 0.3125
- factor_rows: int32 [384, 4], P('row', 'col'), may hold values from 0 to 63
- factor_cols: int32 [384, 4], P('row', 'col'), may hold values from 0 to 255
- diag_cost: float32 [1024, 128], P('col'), may hold values from 0.1 to 1
- linear_cost: float32 [1024, 128], P('col'), may hold values from -6 to 6
- lower_bound: float32 [1536, 128], P('row'), may hold values from -1.5 to -0.2
- upper_bound: float32 [1536, 128], P('row'), may hold values from 0.2 to 1.5
- primal_start: float32 [1024, 128], P('col'), may hold values from -6 to 6
- slack_start: float32 [1536, 128], P('row'), may hold values from -6 to 6
- dual_start: float32 [1536, 128], P('row'), may hold values from -6 to 6
- penalty: float32 [], replicated, may hold values from 3 to 6
Outputs:
- primal_next: float32 [1024, 128], P('col')
- slack_next: float32 [1536, 128], P('row')
- dual_next: float32 [1536, 128], P('row')
- primal_res: float32 [], replicated
- dual_res: float32 [], replicated
The draws below stay inside these ranges and needn't reach their ends.
All inputs are finite; a program needn't handle non-finite values.
Results may differ from the reference program's by a relative error of at most 0.0003.
Values sent between devices are 32-bit elements; how exact they have to be, the bound alone decides.
No kernel may reach another device: no remote copies, remote signals or barrier semaphores. Data moves between devices by JAX's collectives and lax.ppermute only.
A program may use at most 128 MiB of HBM per device.

```python
import math
import jax
import jax.numpy as jnp
from jax import lax

BLK = 128
XB = 256
YB = 192
YG = 64
KA = 96
KG = 48
CG = 6
NX = 1024
NY = 1536
ATILES = 2
GTILES = 3
N_ROW = 8
N_COL = 4


def place_ends(drawn, rng, low, top_value):
    extent = drawn.shape
    index_at = [jax.random.randint(jax.random.fold_in(rng, axis), (), 0, extent[axis]) for axis in range(len(extent))]
    drawn = drawn.at[tuple(index_at)].set(low)
    longest = extent.index(max(extent))
    index_at[longest] = (index_at[longest] + 1) % extent[longest]
    return drawn.at[tuple(index_at)].set(top_value)


def block_scale(rng, shape, cuts, smallest, high):
    level, own = 1.0, jax.random.fold_in(rng, 6)
    for axis_at, parts in cuts:
        steps = jnp.exp(jax.random.uniform(jax.random.fold_in(own, axis_at), (parts,), jnp.float32, smallest / len(cuts), high / len(cuts)))
        level = level * jnp.repeat(steps, shape[axis_at] // parts).reshape([-1 if axis == axis_at else 1 for axis in range(len(shape))])
    return level


def scatter_about(key, extent, scale, reach, split=(), kind=jnp.bfloat16):
    values = scale * jax.random.normal(key, extent, jnp.float32)
    if split:
        values = values * block_scale(key, extent, split, -0.22, 0.18)
    return jnp.clip(values, -reach, reach).astype(kind)


def setup_inputs(seed: int = 0) -> dict:
    key_list = jax.random.split(jax.random.key(seed), 15)
    constraint_tiles = scatter_about(key_list[0], (N_ROW * KA, N_COL, BLK, BLK), (BLK * ATILES) ** -0.5, 0.375, ((0, 8), (1, 4)), jnp.float32)
    constraint_rows = place_ends(jax.random.randint(key_list[1], (N_ROW * KA, N_COL), 0, YB), jax.random.fold_in(key_list[1], 1), 0, YB - 1).astype(jnp.int32)
    constraint_cols = place_ends(jax.random.randint(key_list[2], (N_ROW * KA, N_COL), 0, XB), jax.random.fold_in(key_list[2], 1), 0, XB - 1).astype(jnp.int32)
    factor_tiles = scatter_about(key_list[3], (N_ROW * KG, N_COL, BLK, BLK), (BLK * GTILES) ** -0.5, 0.3125, ((0, 8), (1, 4)), jnp.float32)
    factor_rows = place_ends(jax.random.randint(key_list[4], (N_ROW * KG, N_COL), 0, YG), jax.random.fold_in(key_list[4], 1), 0, YG - 1).astype(jnp.int32)
    factor_cols = place_ends(jax.random.randint(key_list[5], (N_ROW * KG, N_COL), 0, XB), jax.random.fold_in(key_list[5], 1), 0, XB - 1).astype(jnp.int32)
    diag_cost = jnp.clip(jnp.exp(math.log(1.0) - 2.3025851 * jax.random.uniform(key_list[6], (NX, BLK), jnp.float32) ** block_scale(key_list[6], (NX, BLK), ((0, 4),), -0.2, 0.2)), 0.1, 1.0)
    linear_cost = scatter_about(key_list[7], (NX, BLK), 1.0, 6.0, ((0, 4),), jnp.float32)
    lower_bound = jnp.clip(-1.5 + 1.3 * jax.random.uniform(key_list[8], (NY, BLK), jnp.float32) ** block_scale(key_list[8], (NY, BLK), ((0, 8),), -0.2, 0.2), -1.5, -0.2)
    upper_bound = jnp.clip(0.2 + 1.3 * jax.random.uniform(key_list[9], (NY, BLK), jnp.float32) ** block_scale(key_list[9], (NY, BLK), ((0, 8),), -0.2, 0.2), 0.2, 1.5)
    primal_start = scatter_about(key_list[10], (NX, BLK), 1.0, 6.0, ((0, 4),), jnp.float32)
    slack_start = scatter_about(key_list[11], (NY, BLK), 1.0, 6.0, ((0, 8),), jnp.float32)
    dual_start = scatter_about(key_list[12], (NY, BLK), 1.0, 6.0, ((0, 8),), jnp.float32)
    penalty = jnp.clip(jnp.exp(jax.random.uniform(key_list[13], (), jnp.float32, math.log(3.0), math.log(6.0))), 3.0, 6.0)
    return dict(constraint_tiles=constraint_tiles, constraint_rows=constraint_rows, constraint_cols=constraint_cols, factor_tiles=factor_tiles, factor_rows=factor_rows, factor_cols=factor_cols, diag_cost=diag_cost, linear_cost=linear_cost, lower_bound=lower_bound, upper_bound=upper_bound, primal_start=primal_start, slack_start=slack_start, dual_start=dual_start, penalty=penalty)


SIGMA = 1e-6
RELAX = 1.6
HIGH = lax.Precision.HIGHEST


def positions(rows, cols, per_device, row_blocks):
    kidx = jnp.arange(rows.shape[0], dtype=jnp.int32)[:, None] // per_device
    cidx = jnp.arange(rows.shape[1], dtype=jnp.int32)[None, :]
    grow = (kidx * row_blocks + rows).astype(jnp.int32).reshape(-1)
    gcol = (cidx * XB + cols).astype(jnp.int32).reshape(-1)
    return grow, gcol


def forward(tiles, grow, gcol, vec, count):
    prod = jnp.einsum("kij,kj->ki", tiles, vec[gcol], precision=HIGH)
    return jax.ops.segment_sum(prod, grow, num_segments=count)


def backward(tiles, grow, gcol, vec, count):
    prod = jnp.einsum("kij,ki->kj", tiles, vec[grow], precision=HIGH)
    return jax.ops.segment_sum(prod, gcol, num_segments=count)


def reference(constraint_tiles, constraint_rows, constraint_cols, factor_tiles, factor_rows, factor_cols, diag_cost, linear_cost, lower_bound, upper_bound, primal_start, slack_start, dual_start, penalty):
    ctiles = constraint_tiles.reshape(-1, BLK, BLK)
    ftiles = factor_tiles.reshape(-1, BLK, BLK)
    crow, ccol = positions(constraint_rows, constraint_cols, KA, YB)
    frow, fcol = positions(factor_rows, factor_cols, KG, YG)
    nx = XB * N_COL
    ny = YB * N_ROW
    ng = YG * N_ROW
    rho = penalty

    def apply_k(vec):
        avec = forward(ctiles, crow, ccol, vec, ny)
        gvec = forward(ftiles, frow, fcol, vec, ng)
        back = backward(ctiles, crow, ccol, rho * avec, nx) + backward(ftiles, frow, fcol, gvec, nx)
        return (diag_cost + SIGMA) * vec + back

    rhs = SIGMA * primal_start - linear_cost + backward(ctiles, crow, ccol, rho * slack_start - dual_start, nx)
    csq = jax.ops.segment_sum(jnp.sum(ctiles * ctiles, axis=1), ccol, num_segments=nx)
    fsq = jax.ops.segment_sum(jnp.sum(ftiles * ftiles, axis=1), fcol, num_segments=nx)
    precond = diag_cost + SIGMA + fsq + rho * csq
    solution = primal_start
    resid = rhs - apply_k(solution)
    scaled = resid / precond
    direction = scaled
    gamma = jnp.sum(resid * scaled)
    for step in range(CG):
        image = apply_k(direction)
        alpha = gamma / jnp.sum(direction * image)
        solution = solution + alpha * direction
        resid = resid - alpha * image
        scaled = resid / precond
        gamma_new = jnp.sum(resid * scaled)
        direction = scaled + (gamma_new / gamma) * direction
        gamma = gamma_new
    tilde_z = forward(ctiles, crow, ccol, solution, ny)
    primal_next = RELAX * solution + (1.0 - RELAX) * primal_start
    relaxed = RELAX * tilde_z + (1.0 - RELAX) * slack_start
    slack_next = jnp.minimum(jnp.maximum(relaxed + dual_start / rho, lower_bound), upper_bound)
    dual_next = dual_start + rho * (relaxed - slack_next)
    image_next = forward(ctiles, crow, ccol, primal_next, ny)
    gnext = forward(ftiles, frow, fcol, primal_next, ng)
    primal_res = jnp.max(jnp.abs(image_next - slack_next))
    dvec = diag_cost * primal_next + backward(ftiles, frow, fcol, gnext, nx) + linear_cost + backward(ctiles, crow, ccol, dual_next, nx)
    dual_res = jnp.max(jnp.abs(dvec))
    return primal_next, slack_next, dual_next, primal_res, dual_res
```

```python
import functools

import jax
import jax.numpy as jnp
from jax import lax
from jax.experimental import pallas as pl
from jax.experimental.pallas import tpu as pltpu
from jax.sharding import PartitionSpec as P

YG = 64
CG = 6

SIGMA = 1e-06
RELAX = 1.6

F32 = jnp.float32
BF16 = jnp.bfloat16
LANES = 128
GROUP = 4
VMEM_LIMIT = 24 * 1024 * 1024


def dot(a, b):
    return lax.dot_general(a, b, (((1,), (0,)), ((), ())), preferred_element_type=F32)


def dot_t(a, b):
    return lax.dot_general(a, b, (((1,), (1,)), ((), ())), preferred_element_type=F32)


def split3(x):
    high = x.astype(BF16)
    rest = x - high.astype(F32)
    mid = rest.astype(BF16)
    low = (rest - mid.astype(F32)).astype(BF16)
    return high, mid, low


def tree(parts, op=jnp.add):
    parts = list(parts)
    while len(parts) > 1:
        parts = [op(parts[i], parts[i + 1]) for i in range(0, len(parts), 2)]
    return parts[0]


def row_sum(x):
    return jnp.sum(x, axis=0, keepdims=True)


def pad_rows(rows):
    return jnp.concatenate(list(rows) + [jnp.zeros((8 - len(rows), LANES), F32)], axis=0)


def gather(onehot_ref, x):
    return dot(onehot_ref[...], jnp.concatenate(split3(x), axis=0))


def scatter(onehot, x):
    high, mid, low = split3(x)
    return dot(onehot, high) + (dot(onehot, mid) + dot(onehot, low))


def run_tiles(w_ref, l_ref, r0_ref, r1_ref, product):
    pairs = w_ref.shape[0]
    blocks = pairs // 2
    unroll = next(n for n in (4, 3, 2, 1) if blocks % n == 0)

    def body(step, carry):
        for inner in range(unroll):
            block = step * unroll + inner
            at = pl.multiple_of(block * 16, 16)
            left = l_ref[pl.ds(at, 16), :]
            first = product(left, w_ref[2 * block])
            second = product(left, w_ref[2 * block + 1])
            r0_ref[pl.ds(at, 8), :] = first[:8, :LANES]
            r1_ref[pl.ds(at, 8), :] = first[:8, LANES:]
            r0_ref[pl.ds(pl.multiple_of(at + 8, 8), 8), :] = second[8:, :LANES]
            r1_ref[pl.ds(pl.multiple_of(at + 8, 8), 8), :] = second[8:, LANES:]
        return carry

    lax.fori_loop(0, blocks // unroll, body, 0)


def forward_parts(vec, gf_ref, w_ref, l_ref, r0_ref, r1_ref):
    picked = gather(gf_ref, vec)
    first = lax.broadcasted_iota(jnp.int32, picked.shape, 0) % (2 * GROUP) < GROUP
    zero = jnp.zeros_like(picked)
    l_ref[:, :LANES] = jnp.where(first, picked, zero).astype(BF16)
    l_ref[:, LANES:] = jnp.where(first, zero, picked).astype(BF16)
    run_tiles(w_ref, l_ref, r0_ref, r1_ref, dot_t)
    count = 2 * w_ref.shape[0]
    out = None
    for part in (2, 1, 0):
        at = pl.ds(part, count, stride=GROUP)
        term = r0_ref[at, :] + r1_ref[at, :]
        out = term if out is None else out + term
    return out


def backward_sum(vec, gb_ref, sb_ref, w_ref, l_ref, r0_ref, r1_ref):
    picked = gather(gb_ref, vec).astype(BF16)
    l_ref[:, :LANES] = picked
    l_ref[:, LANES:] = picked
    run_tiles(w_ref, l_ref, r0_ref, r1_ref, dot)
    half = w_ref.shape[0]
    even, odd = None, None
    for part in (2, 1, 0):
        one = r0_ref[pl.ds(part, half, stride=2 * GROUP), :]
        two = r1_ref[pl.ds(GROUP + part, half, stride=2 * GROUP), :]
        even = one if even is None else even + one
        odd = two if odd is None else odd + two
    return scatter(sb_ref[...], jnp.concatenate([even, odd], axis=0))


def gathered_rows(part_refs, s_ref):
    count = s_ref.shape[2]
    return tree(scatter(s_ref[j], ref[:count, :]) for j, ref in enumerate(part_refs))


def init_kernel(a_steps, a_ref, g_ref, w_ref, sq_ref):
    step = pl.program_id(0)

    def convert(ref):
        for t in range(ref.shape[0]):
            tile = ref[t]
            high = tile.astype(BF16)
            low = (tile - high.astype(F32)).astype(BF16)
            at = (t % 2) * LANES
            w_ref[t // 2, :LANES, at : at + LANES] = high
            w_ref[t // 2, LANES:, at : at + LANES] = low
            sq_ref[t : t + 1, :] = row_sum(tile * tile)

    @pl.when(step < a_steps)
    def _():
        convert(a_ref)

    @pl.when(step >= a_steps)
    def _():
        convert(g_ref)


def first_forward_kernel(v_ref, gf_ref, w_ref, out_ref, l_ref, r0_ref, r1_ref):
    count = 2 * w_ref.shape[0]
    out_ref[:count, :] = forward_parts(v_ref[...], gf_ref, w_ref, l_ref, r0_ref, r1_ref)
    out_ref[count:, :] = jnp.zeros((8, LANES), F32)


def first_backward_kernel(n_col, ycount, acount, *refs):
    rho_ref, *refs = refs
    part_refs, refs = refs[:n_col], refs[n_col:]
    s_ref, gb_ref, sb_ref, w_ref, sq_ref, slack_ref, dual_ref, z_ref, y_ref, l_ref, r0_ref, r1_ref = refs
    rho = rho_ref[0]
    full = gathered_rows(part_refs, s_ref)
    y_ref[...] = full
    top = rho * slack_ref[...] - dual_ref[...] - rho * full[:ycount]
    vec = jnp.concatenate([top, -full[ycount:]], axis=0)
    xcount = sb_ref.shape[0]
    z_ref[:xcount, :] = backward_sum(vec, gb_ref, sb_ref, w_ref, l_ref, r0_ref, r1_ref)
    half = w_ref.shape[0]
    squares = jnp.concatenate([sq_ref[pl.ds(0, half, stride=2), :], sq_ref[pl.ds(1, half, stride=2), :]], axis=0)
    place = lax.broadcasted_iota(jnp.int32, squares.shape, 0)
    place = jnp.where(place < half, 2 * place, 2 * (place - half) + 1)
    squares = jnp.where(place < acount, rho * squares, squares)
    z_ref[xcount:, :] = scatter(sb_ref[...], squares)


def finish_forward(u, p, resid, shifted, out_ref, gf_ref, w_ref, l_ref, r0_ref, r1_ref):
    count = 2 * w_ref.shape[0]
    weighted = shifted * u
    rows = [row_sum(resid * u), row_sum(weighted * u)]
    if p is not None:
        rows.append(row_sum(weighted * p))
    out_ref[count:, :] = pad_rows(rows)
    out_ref[:count, :] = forward_parts(u, gf_ref, w_ref, l_ref, r0_ref, r1_ref)


def second_forward_kernel(n_plane, *refs):
    z_refs, refs = refs[:n_plane], refs[n_plane:]
    v_ref, d_ref, c_ref, gf_ref, w_ref, r_ref, u_ref, pre_ref, out_ref, l_ref, r0_ref, r1_ref = refs
    xcount = v_ref.shape[0]
    total = tree(ref[...] for ref in z_refs)
    v, d = v_ref[...], d_ref[...]
    resid = total[:xcount] - c_ref[...] - d * v
    shifted = d + SIGMA
    pre = shifted + total[xcount:]
    u = resid / pre
    r_ref[...] = resid
    u_ref[...] = u
    pre_ref[...] = pre
    finish_forward(u, None, resid, shifted, out_ref, gf_ref, w_ref, l_ref, r0_ref, r1_ref)


def step_scalars(first, part_refs, sc_old_ref, count):
    totals = jnp.sum(tree(ref[count:, :] for ref in part_refs), axis=1, keepdims=True)
    gamma, one, two = totals[0:1], totals[1:2], totals[2:3]
    if first:
        return gamma, jnp.zeros_like(gamma), one
    old = sc_old_ref[...]
    beta = gamma / old[0:1, 0:1]
    return gamma, beta, one + beta * (2.0 * two + beta * old[2:3, 0:1])


def wide(x):
    return jnp.broadcast_to(x, (1, LANES))


def backward_kernel(n_col, ycount, first, last, *refs):
    rho_ref, *refs = refs
    part_refs, refs = refs[:n_col], refs[n_col:]
    s_ref, refs = refs[0], refs[1:]
    sc_old_ref = None
    if not first:
        (yp_old_ref, yv_old_ref, sc_old_ref, alpha_ref), refs = refs[:4], refs[4:]
    else:
        (yv_old_ref,), refs = refs[:1], refs[1:]
    if not last:
        (gb_ref, sb_ref, w_ref), refs = refs[:3], refs[3:]
    z_ref, yp_ref, yv_ref, sc_ref, *scratch = refs
    rho = rho_ref[0]
    full = gathered_rows(part_refs, s_ref)
    gamma, beta, pdp = step_scalars(first, part_refs, sc_old_ref, s_ref.shape[2])
    sc_ref[...] = pad_rows([wide(gamma), wide(beta), wide(pdp)])
    if first:
        yp = full
        yv_ref[...] = yv_old_ref[...]
    else:
        yp_old = yp_old_ref[...]
        yp = full + beta * yp_old
        yv_ref[...] = yv_old_ref[...] + alpha_ref[0:1, 0:1] * yp_old
    yp_ref[...] = yp
    scaled = jnp.concatenate([rho * yp[:ycount], yp[ycount:]], axis=0)
    norm = pad_rows([row_sum(scaled * yp)])
    if last:
        z_ref[...] = norm
    else:
        xcount = sb_ref.shape[0]
        z_ref[xcount:, :] = norm
        z_ref[:xcount, :] = backward_sum(scaled, gb_ref, sb_ref, w_ref, *scratch)


def step_alpha(extra, sc_ref):
    norm = jnp.sum(extra[0:1], axis=1, keepdims=True)
    return sc_ref[0:1, 0:1] / (sc_ref[2:3, 0:1] + norm)


def forward_kernel(n_plane, first, *refs):
    z_refs, refs = refs[:n_plane], refs[n_plane:]
    if not first:
        p_old_ref, refs = refs[0], refs[1:]
    (u_old_ref, v_old_ref, r_old_ref, d_ref, pre_ref, sc_ref, gf_ref, w_ref), refs = refs[:8], refs[8:]
    p_ref, v_ref, r_ref, u_ref, alpha_ref, out_ref, *scratch = refs
    xcount = d_ref.shape[0]
    total = tree(ref[...] for ref in z_refs)
    alpha = step_alpha(total[xcount:], sc_ref)
    p = u_old_ref[...]
    if not first:
        p = p + sc_ref[1:2, 0:1] * p_old_ref[...]
    shifted = d_ref[...] + SIGMA
    resid = r_old_ref[...] - alpha * (shifted * p + total[:xcount])
    u = resid / pre_ref[...]
    p_ref[...] = p
    v_ref[...] = v_old_ref[...] + alpha * p
    r_ref[...] = resid
    u_ref[...] = u
    alpha_ref[...] = jnp.broadcast_to(alpha, (8, LANES))
    finish_forward(u, p, resid, shifted, out_ref, gf_ref, w_ref, *scratch)


def final_kernel(n_plane, ycount, *refs):
    rho_ref, *refs = refs
    t_refs, refs = refs[:n_plane], refs[n_plane:]
    (u_ref, p_old_ref, v_ref, start_ref, sc_ref, yp_ref, yv_ref, y0_ref), refs = refs[:8], refs[8:]
    (slack_ref, dual_ref, lower_ref, upper_ref, gb_ref, sb_ref, w_ref), refs = refs[:7], refs[7:]
    primal_out, slack_out, dual_out, z_ref, *scratch = refs
    rho = rho_ref[0]
    alpha = step_alpha(tree(ref[...] for ref in t_refs), sc_ref)
    p = u_ref[...] + sc_ref[1:2, 0:1] * p_old_ref[...]
    v = v_ref[...] + alpha * p
    primal_out[...] = RELAX * v + (1.0 - RELAX) * start_ref[...]
    image = yv_ref[...] + alpha * yp_ref[...]
    image_next = RELAX * image + (1.0 - RELAX) * y0_ref[...]
    dual = dual_ref[...]
    relaxed = RELAX * image[:ycount] + (1.0 - RELAX) * slack_ref[...]
    slack_next = jnp.minimum(jnp.maximum(relaxed + dual / rho, lower_ref[...]), upper_ref[...])
    dual_next = dual + rho * (relaxed - slack_next)
    slack_out[...] = slack_next
    dual_out[...] = dual_next
    xcount = sb_ref.shape[0]
    worst = jnp.max(jnp.abs(image_next[:ycount] - slack_next), axis=0, keepdims=True)
    z_ref[xcount:, :] = jnp.broadcast_to(worst, (8, LANES))
    vec = jnp.concatenate([dual_next, image_next[ycount:]], axis=0)
    z_ref[:xcount, :] = backward_sum(vec, gb_ref, sb_ref, w_ref, *scratch)


def residual_kernel(n_plane, *refs):
    z_refs, (primal_ref, d_ref, c_ref, out_ref) = refs[:n_plane], refs[n_plane:]
    xcount = d_ref.shape[0]
    total = tree(ref[:xcount, :] for ref in z_refs)
    primal = tree((ref[xcount:, :] for ref in z_refs), jnp.maximum)
    dvec = d_ref[...] * primal_ref[...] + total + c_ref[...]
    worst = jnp.max(jnp.abs(dvec), axis=0, keepdims=True)
    out_ref[...] = jnp.concatenate([primal[:4], jnp.broadcast_to(worst, (4, LANES))], axis=0)


VMEM_SPEC = pl.BlockSpec(memory_space=pltpu.VMEM)
SMEM_SPEC = pl.BlockSpec(memory_space=pltpu.SMEM)


def call(kernel, name, outs, args, scratch=(), scalar=False):
    specs = [SMEM_SPEC if scalar and i == 0 else VMEM_SPEC for i in range(len(args))]
    shapes = tuple(jax.ShapeDtypeStruct(s, F32) for s in outs)
    return pl.pallas_call(
        kernel,
        out_shape=shapes,
        in_specs=specs,
        out_specs=tuple(VMEM_SPEC for _ in outs),
        scratch_shapes=list(scratch),
        compiler_params=pltpu.CompilerParams(vmem_limit_bytes=VMEM_LIMIT),
        name=name,
    )(*args)


def swap(x, axis, size, distance):
    return lax.ppermute(x, axis, [(i, i ^ distance) for i in range(size)])


def exchange(x, axis, size, distances):
    return [x] + [swap(x, axis, size, m) for m in distances]


def local(n_row, n_col, *args):
    (
        constraint_tiles,
        constraint_rows,
        constraint_cols,
        factor_tiles,
        factor_rows,
        factor_cols,
        diag_cost,
        linear_cost,
        lower_bound,
        upper_bound,
        primal_start,
        slack_start,
        dual_start,
        penalty,
    ) = args
    width = constraint_tiles.shape[2]
    ctiles = constraint_tiles.reshape(-1, width, width)
    ftiles = factor_tiles.reshape(-1, width, width)
    acount, fcount = ctiles.shape[0], ftiles.shape[0]
    count = acount + fcount
    pairs = count // 2
    xcount = primal_start.shape[0]
    ycount = slack_start.shape[0]
    full = ycount + YG
    rho = penalty.reshape(1)

    def over_col(x):
        return exchange(x, "col", n_col, range(1, n_col))

    def over_row(x, op=jnp.add):
        chip = op(x, swap(x, "row", n_row, 1))
        return exchange(chip, "row", n_row, range(2, n_row, 2))

    xat = jnp.concatenate([constraint_cols.reshape(-1), factor_cols.reshape(-1)])
    yat = jnp.concatenate([constraint_rows.reshape(-1), ycount + factor_rows.reshape(-1)])
    part = jnp.arange(GROUP * count, dtype=jnp.int32) % GROUP

    def pick(at, size):
        place = jnp.where(part < 3, part * size + jnp.repeat(at, GROUP), -1)
        return (place[:, None] == jnp.arange(3 * size, dtype=jnp.int32)[None, :]).astype(BF16)

    def place(at, size):
        return (jnp.arange(size, dtype=jnp.int32)[:, None] == at[None, :]).astype(BF16)

    gf = pick(xat, xcount)
    gb = pick(yat, full)
    sb = place(jnp.concatenate([xat[0::2], xat[1::2]]), xcount)
    s_all = jnp.stack([place(at, full) for at in over_col(yat)])

    block = 8
    a_steps, f_steps = acount // block, fcount // block
    tiles, squares = pl.pallas_call(
        functools.partial(init_kernel, a_steps),
        grid=(a_steps + f_steps,),
        in_specs=[
            pl.BlockSpec((block, width, width), lambda i: (jnp.minimum(i, a_steps - 1), 0, 0)),
            pl.BlockSpec((block, width, width), lambda i: (jnp.maximum(i - a_steps, 0), 0, 0)),
        ],
        out_specs=(
            pl.BlockSpec((block // 2, 2 * width, 2 * width), lambda i: (i, 0, 0)),
            pl.BlockSpec((block, width), lambda i: (i, 0)),
        ),
        out_shape=(
            jax.ShapeDtypeStruct((pairs, 2 * width, 2 * width), BF16),
            jax.ShapeDtypeStruct((count, width), F32),
        ),
        compiler_params=pltpu.CompilerParams(vmem_limit_bytes=VMEM_LIMIT),
        name="split_tiles",
    )(ctiles, ftiles)

    scratch = (
        pltpu.VMEM((GROUP * count, 2 * width), BF16),
        pltpu.VMEM((GROUP * count, width), F32),
        pltpu.VMEM((GROUP * count, width), F32),
    )
    xs, ys, small = (xcount, width), (full, width), (8, width)
    sent, summed = (count + 8, width), (xcount + 8, width)

    (parts,) = call(first_forward_kernel, "first_forward", [sent], (primal_start, gf, tiles), scratch)
    z, y0 = call(
        functools.partial(first_backward_kernel, n_col, ycount, acount),
        "first_backward",
        [(2 * xcount, width), ys],
        (rho, *over_col(parts), s_all, gb, sb, tiles, squares, slack_start, dual_start),
        scratch,
        scalar=True,
    )
    zs = over_row(z)
    resid, u, precond, parts = call(
        functools.partial(second_forward_kernel, len(zs)),
        "second_forward",
        [xs, xs, xs, sent],
        (*zs, primal_start, diag_cost, linear_cost, gf, tiles),
        scratch,
    )
    v, yv = primal_start, y0
    p = yp = sc = alpha = None
    for step in range(CG):
        first, last = step == 0, step + 1 == CG
        state = (yv,) if first else (yp, yv, sc, alpha)
        mats = () if last else (gb, sb, tiles)
        z, yp, yv, sc = call(
            functools.partial(backward_kernel, n_col, ycount, first, last),
            "last_norm" if last else "backward",
            [small if last else summed, ys, ys, small],
            (rho, *over_col(parts), s_all, *state, *mats),
            () if last else scratch,
            scalar=True,
        )
        zs = over_row(z)
        if not last:
            p, v, resid, u, alpha, parts = call(
                functools.partial(forward_kernel, len(zs), first),
                "forward",
                [xs, xs, xs, xs, small, sent],
                (*zs, *(() if first else (p,)), u, v, resid, diag_cost, precond, sc, gf, tiles),
                scratch,
            )
    primal_next, slack_next, dual_next, z = call(
        functools.partial(final_kernel, len(zs), ycount),
        "final",
        [xs, (ycount, width), (ycount, width), summed],
        (rho, *zs, u, p, v, primal_start, sc, yp, yv, y0)
        + (slack_start, dual_start, lower_bound, upper_bound, gb, sb, tiles),
        scratch,
        scalar=True,
    )

    def join(a, b):
        is_sum = lax.broadcasted_iota(jnp.int32, a.shape, 0) < xcount
        return jnp.where(is_sum, a + b, jnp.maximum(a, b))

    zs = over_row(z, join)
    (worst,) = call(
        functools.partial(residual_kernel, len(zs)),
        "residuals",
        [small],
        (*zs, primal_next, diag_cost, linear_cost),
    )
    worst = tree(over_col(worst), jnp.maximum)
    return (primal_next, slack_next, dual_next, jnp.max(worst[:4]), jnp.max(worst[4:]))


def solution(mesh):
    placed = (
        P("row", "col", None, None),
        P("row", "col"),
        P("row", "col"),
        P("row", "col", None, None),
        P("row", "col"),
        P("row", "col"),
        P("col", None),
        P("col", None),
        P("row", None),
        P("row", None),
        P("col", None),
        P("row", None),
        P("row", None),
        P(),
    )
    return jax.shard_map(
        functools.partial(local, mesh.shape["row"], mesh.shape["col"]),
        mesh=mesh,
        in_specs=placed,
        out_specs=(P("col", None), P("row", None), P("row", None), P(), P()),
        check_vma=False,
    )
```

```python
import functools

import jax
import jax.numpy as jnp
from jax import lax
from jax.experimental import pallas as pl
from jax.experimental.pallas import tpu as pltpu
from jax.sharding import PartitionSpec as P

YG = 64
CG = 6

SIGMA = 1e-06
RELAX = 1.6

F32 = jnp.float32
BF16 = jnp.bfloat16
LANES = 128
PARTS = 2
SHARED = 16 // (2 * PARTS)
VMEM_LIMIT = 24 * 1024 * 1024


def dot(a, b):
    return lax.dot_general(a, b, (((1,), (0,)), ((), ())), preferred_element_type=F32)


def split3(x):
    high = x.astype(BF16)
    rest = x - high.astype(F32)
    mid = rest.astype(BF16)
    low = (rest - mid.astype(F32)).astype(BF16)
    return high, mid, low


def split2(x):
    high = x.astype(BF16)
    return high, (x - high.astype(F32)).astype(BF16)


def tree(parts, op=jnp.add):
    parts = list(parts)
    while len(parts) > 1:
        parts = [op(parts[i], parts[i + 1]) for i in range(0, len(parts), 2)]
    return parts[0]


def row_sum(x):
    return jnp.sum(x, axis=0, keepdims=True)


def half_sum(x):
    half = x.shape[0] // 2
    return row_sum(x[:half]) + row_sum(x[half:])


def pad_rows(rows):
    return jnp.concatenate(list(rows) + [jnp.zeros((8 - len(rows), LANES), F32)], axis=0)


def gather(onehot_ref, x):
    return dot(onehot_ref[...], jnp.concatenate(split2(x), axis=0))


def scatter(onehot, x, split=split2):
    return tree(dot(onehot, part) for part in split(x)) if split is split2 else sum(dot(onehot, p) for p in split(x))


def run_tiles(w_ref, l_ref, r0_ref, r1_ref):
    blocks = w_ref.shape[0] // SHARED
    unroll = next(n for n in (6, 4, 3, 2, 1) if blocks % n == 0)
    rows = 2 * PARTS

    def body(step, carry):
        for inner in range(unroll):
            block = step * unroll + inner
            at = pl.multiple_of(block * 16, 16)
            left = l_ref[pl.ds(at, 16), :]
            for k in range(SHARED):
                out = dot(left, w_ref[SHARED * block + k])[k * rows : (k + 1) * rows]
                r0_ref[pl.ds(at + k * rows, rows), :] = out[:, :LANES]
                r1_ref[pl.ds(at + k * rows, rows), :] = out[:, LANES:]
        return carry

    lax.fori_loop(0, blocks // unroll, body, 0)


def forward_parts(vec, gf_ref, wt_ref, l_ref, r0_ref, r1_ref):
    picked = gather(gf_ref, vec)
    first = lax.broadcasted_iota(jnp.int32, picked.shape, 0) % (2 * PARTS) < PARTS
    zero = jnp.zeros_like(picked)
    l_ref[:, :LANES] = jnp.where(first, picked, zero).astype(BF16)
    l_ref[:, LANES:] = jnp.where(first, zero, picked).astype(BF16)
    run_tiles(wt_ref, l_ref, r0_ref, r1_ref)
    count = 2 * wt_ref.shape[0]
    terms = []
    for part in range(PARTS):
        at = pl.ds(part, count, stride=PARTS)
        terms.append(r0_ref[at, :] + r1_ref[at, :])
    return tree(terms)


def backward_sum(vec, gb_ref, sb_ref, w_ref, l_ref, r0_ref, r1_ref):
    picked = gather(gb_ref, vec).astype(BF16)
    l_ref[:, :LANES] = picked
    l_ref[:, LANES:] = picked
    run_tiles(w_ref, l_ref, r0_ref, r1_ref)
    half = w_ref.shape[0]
    even = tree(r0_ref[pl.ds(part, half, stride=2 * PARTS), :] for part in range(PARTS))
    odd = tree(r1_ref[pl.ds(PARTS + part, half, stride=2 * PARTS), :] for part in range(PARTS))
    return scatter(sb_ref[...], jnp.concatenate([even, odd], axis=0))


def gathered_rows(part_refs, s_ref):
    count = s_ref.shape[2]
    return tree(scatter(s_ref[j], ref[:count, :]) for j, ref in enumerate(part_refs))


def put_halves(refs, total, extra):
    half = total.shape[0] // 2
    for ref, part in zip(refs, (total[:half], total[half:])):
        ref[:half, :] = part
        ref[half:, :] = extra


def init_kernel(a_steps, a_ref, g_ref, w_ref, wt_ref, sq_ref):
    step = pl.program_id(0)

    def convert(ref):
        for t in range(ref.shape[0]):
            tile = ref[t]
            at = (t % 2) * LANES
            high, low = split2(tile)
            w_ref[t // 2, :LANES, at : at + LANES] = high
            w_ref[t // 2, LANES:, at : at + LANES] = low
            high, low = split2(tile.T)
            wt_ref[t // 2, at : at + LANES, :LANES] = high
            wt_ref[t // 2, at : at + LANES, LANES:] = low
            sq_ref[t : t + 1, :] = row_sum(tile * tile)

    @pl.when(step < a_steps)
    def _():
        convert(a_ref)

    @pl.when(step >= a_steps)
    def _():
        convert(g_ref)


def first_forward_kernel(v_ref, at_ref, gf_ref, w_ref, out_ref, l_ref, r0_ref, r1_ref):
    count = 2 * w_ref.shape[0]
    out_ref[:count, :] = forward_parts(v_ref[...], gf_ref, w_ref, l_ref, r0_ref, r1_ref)
    out_ref[count:, :] = at_ref[...]


def first_backward_kernel(n_col, ycount, acount, *refs):
    rho_ref, *refs = refs
    part_refs, refs = refs[:n_col], refs[n_col:]
    (gb_ref, sb_ref, w_ref, sq_ref, slack_ref, dual_ref), refs = refs[:6], refs[6:]
    mine_ref, theirs_ref, y_ref, s_ref, l_ref, r0_ref, r1_ref = refs
    rho = rho_ref[0]
    _, full_rows, count = s_ref.shape
    for j, ref in enumerate(part_refs):
        for row in range(pl.cdiv(count, LANES)):
            size = min(LANES, count - row * LANES)
            at = ref[count + row : count + row + 1, :size].astype(jnp.int32)
            hit = lax.broadcasted_iota(jnp.int32, (full_rows, size), 0) == at
            s_ref[j, :, row * LANES : row * LANES + size] = jnp.where(hit, 1.0, 0.0).astype(BF16)
    full = gathered_rows(part_refs, s_ref)
    y_ref[...] = full
    top = rho * slack_ref[...] - dual_ref[...] - rho * full[:ycount]
    vec = jnp.concatenate([top, -full[ycount:]], axis=0)
    total = backward_sum(vec, gb_ref, sb_ref, w_ref, l_ref, r0_ref, r1_ref)
    half = w_ref.shape[0]
    squares = jnp.concatenate([sq_ref[pl.ds(0, half, stride=2), :], sq_ref[pl.ds(1, half, stride=2), :]], axis=0)
    place = lax.broadcasted_iota(jnp.int32, squares.shape, 0)
    place = jnp.where(place < half, 2 * place, 2 * (place - half) + 1)
    squares = jnp.where(place < acount, rho * squares, squares)
    squares = scatter(sb_ref[...], squares, split3)
    half = total.shape[0] // 2
    mine_ref[:half, :] = total[:half]
    mine_ref[half:, :] = squares[:half]
    theirs_ref[:half, :] = total[half:]
    theirs_ref[half:, :] = squares[half:]


def finish_forward(u, p, resid, shifted, out_ref, gf_ref, w_ref, l_ref, r0_ref, r1_ref):
    count = 2 * w_ref.shape[0]
    weighted = shifted * u
    rows = [half_sum(resid * u), half_sum(weighted * u)]
    if p is not None:
        rows.append(half_sum(weighted * p))
    out_ref[count:, :] = pad_rows(rows)
    out_ref[:count, :] = forward_parts(u, gf_ref, w_ref, l_ref, r0_ref, r1_ref)


def second_forward_kernel(*refs):
    (mine_ref, theirs_ref), refs = refs[:2], refs[2:]
    v_ref, d_ref, c_ref, gf_ref, w_ref, r_ref, u_ref, pre_ref, out_ref, l_ref, r0_ref, r1_ref = refs
    half = v_ref.shape[0] // 2
    total = jnp.concatenate([mine_ref[:half, :], theirs_ref[:half, :]], axis=0)
    squares = jnp.concatenate([mine_ref[half:, :], theirs_ref[half:, :]], axis=0)
    v, d = v_ref[...], d_ref[...]
    resid = total - c_ref[...] - d * v
    shifted = d + SIGMA
    pre = shifted + squares
    u = resid / pre
    r_ref[...] = resid
    u_ref[...] = u
    pre_ref[...] = pre
    finish_forward(u, None, resid, shifted, out_ref, gf_ref, w_ref, l_ref, r0_ref, r1_ref)


def step_scalars(first, part_refs, sc_old_ref, count):
    totals = jnp.sum(tree(ref[count:, :] for ref in part_refs), axis=1, keepdims=True)
    gamma, one, two = totals[0:1], totals[1:2], totals[2:3]
    if first:
        return gamma, jnp.zeros_like(gamma), one
    old = sc_old_ref[...]
    beta = gamma / old[0:1, 0:1]
    return gamma, beta, one + beta * (2.0 * two + beta * old[2:3, 0:1])


def wide(x):
    return jnp.broadcast_to(x, (1, LANES))


def backward_kernel(n_col, ycount, first, last, *refs):
    rho_ref, *refs = refs
    part_refs, refs = refs[:n_col], refs[n_col:]
    s_ref, refs = refs[0], refs[1:]
    sc_old_ref = None
    if not first:
        (yp_old_ref, yv_old_ref, sc_old_ref, alpha_ref), refs = refs[:4], refs[4:]
    else:
        (yv_old_ref,), refs = refs[:1], refs[1:]
    if not last:
        (gb_ref, sb_ref, w_ref), refs = refs[:3], refs[3:]
    if last:
        z_ref, *refs = refs
    else:
        mine_ref, theirs_ref, *refs = refs
    yp_ref, yv_ref, sc_ref, *scratch = refs
    rho = rho_ref[0]
    full = gathered_rows(part_refs, s_ref)
    gamma, beta, pdp = step_scalars(first, part_refs, sc_old_ref, s_ref.shape[2])
    sc_ref[...] = pad_rows([wide(gamma), wide(beta), wide(pdp)])
    if first:
        yp = full
        yv_ref[...] = yv_old_ref[...]
    else:
        yp_old = yp_old_ref[...]
        yp = full + beta * yp_old
        yv_ref[...] = yv_old_ref[...] + alpha_ref[0:1, 0:1] * yp_old
    yp_ref[...] = yp
    scaled = jnp.concatenate([rho * yp[:ycount], yp[ycount:]], axis=0)
    norm = pad_rows([row_sum(scaled * yp)])
    if last:
        z_ref[...] = norm
    else:
        put_halves((mine_ref, theirs_ref), backward_sum(scaled, gb_ref, sb_ref, w_ref, *scratch), norm)


def step_alpha(extra, sc_ref):
    norm = jnp.sum(extra[0:1], axis=1, keepdims=True)
    return sc_ref[0:1, 0:1] / (sc_ref[2:3, 0:1] + norm)


def forward_kernel(first, *refs):
    (mine_ref, theirs_ref), refs = refs[:2], refs[2:]
    if not first:
        p_old_ref, refs = refs[0], refs[1:]
    (u_old_ref, v_old_ref, r_old_ref, d_ref, pre_ref, sc_ref, gf_ref, w_ref), refs = refs[:8], refs[8:]
    p_ref, v_ref, r_ref, u_ref, alpha_ref, out_ref, *scratch = refs
    half = d_ref.shape[0] // 2
    total = jnp.concatenate([mine_ref[:half, :], theirs_ref[:half, :]], axis=0)
    alpha = step_alpha(mine_ref[half:, :], sc_ref)
    p = u_old_ref[...]
    if not first:
        p = p + sc_ref[1:2, 0:1] * p_old_ref[...]
    shifted = d_ref[...] + SIGMA
    resid = r_old_ref[...] - alpha * (shifted * p + total)
    u = resid / pre_ref[...]
    p_ref[...] = p
    v_ref[...] = v_old_ref[...] + alpha * p
    r_ref[...] = resid
    u_ref[...] = u
    alpha_ref[...] = jnp.broadcast_to(alpha, (8, LANES))
    finish_forward(u, p, resid, shifted, out_ref, gf_ref, w_ref, *scratch)


def final_kernel(ycount, *refs):
    rho_ref, t_ref, *refs = refs
    (u_ref, p_old_ref, v_ref, start_ref, sc_ref, yp_ref, yv_ref, y0_ref), refs = refs[:8], refs[8:]
    (slack_ref, dual_ref, lower_ref, upper_ref, gb_ref, sb_ref, w_ref), refs = refs[:7], refs[7:]
    primal_out, slack_out, dual_out, mine_ref, theirs_ref, *scratch = refs
    rho = rho_ref[0]
    alpha = step_alpha(t_ref[...], sc_ref)
    p = u_ref[...] + sc_ref[1:2, 0:1] * p_old_ref[...]
    v = v_ref[...] + alpha * p
    primal_out[...] = RELAX * v + (1.0 - RELAX) * start_ref[...]
    image = yv_ref[...] + alpha * yp_ref[...]
    image_next = RELAX * image + (1.0 - RELAX) * y0_ref[...]
    dual = dual_ref[...]
    relaxed = RELAX * image[:ycount] + (1.0 - RELAX) * slack_ref[...]
    slack_next = jnp.minimum(jnp.maximum(relaxed + dual / rho, lower_ref[...]), upper_ref[...])
    dual_next = dual + rho * (relaxed - slack_next)
    slack_out[...] = slack_next
    dual_out[...] = dual_next
    worst = jnp.max(jnp.abs(image_next[:ycount] - slack_next), axis=0, keepdims=True)
    vec = jnp.concatenate([dual_next, image_next[ycount:]], axis=0)
    total = backward_sum(vec, gb_ref, sb_ref, w_ref, *scratch)
    put_halves((mine_ref, theirs_ref), total, jnp.broadcast_to(worst, (8, LANES)))


def residual_kernel(z_ref, primal_ref, d_ref, c_ref, out_ref):
    half = d_ref.shape[0] // 2
    dvec = d_ref[:half, :] * primal_ref[:half, :] + z_ref[:half, :] + c_ref[:half, :]
    worst = jnp.max(jnp.abs(dvec), axis=0, keepdims=True)
    out_ref[...] = jnp.concatenate([z_ref[half : half + 4, :], jnp.broadcast_to(worst, (4, LANES))], axis=0)


VMEM_SPEC = pl.BlockSpec(memory_space=pltpu.VMEM)
SMEM_SPEC = pl.BlockSpec(memory_space=pltpu.SMEM)


def call(kernel, name, outs, args, scratch=(), scalar=False):
    specs = [SMEM_SPEC if scalar and i == 0 else VMEM_SPEC for i in range(len(args))]
    shapes = tuple(s if isinstance(s, jax.ShapeDtypeStruct) else jax.ShapeDtypeStruct(s, F32) for s in outs)
    return pl.pallas_call(
        kernel,
        out_shape=shapes,
        in_specs=specs,
        out_specs=tuple(VMEM_SPEC for _ in outs),
        scratch_shapes=list(scratch),
        compiler_params=pltpu.CompilerParams(vmem_limit_bytes=VMEM_LIMIT),
        name=name,
    )(*args)


def swap(x, axis, size, distance):
    return lax.ppermute(x, axis, [(i, i ^ distance) for i in range(size)])


def exchange(x, axis, size, distances):
    return [x] + [swap(x, axis, size, m) for m in distances]


def local(n_row, n_col, *args):
    (
        constraint_tiles,
        constraint_rows,
        constraint_cols,
        factor_tiles,
        factor_rows,
        factor_cols,
        diag_cost,
        linear_cost,
        lower_bound,
        upper_bound,
        primal_start,
        slack_start,
        dual_start,
        penalty,
    ) = args
    width = constraint_tiles.shape[2]
    ctiles = constraint_tiles.reshape(-1, width, width)
    ftiles = factor_tiles.reshape(-1, width, width)
    acount, fcount = ctiles.shape[0], ftiles.shape[0]
    count = acount + fcount
    pairs = count // 2
    xcount = primal_start.shape[0]
    ycount = slack_start.shape[0]
    full = ycount + YG
    rho = penalty.reshape(1)

    half = xcount // 2
    odd_core = lax.axis_index("row") % 2 == 1

    def turn(x):
        return jnp.where(odd_core, jnp.concatenate([x[half:], x[:half]], axis=0), x)

    diag_cost, linear_cost, primal_start = turn(diag_cost), turn(linear_cost), turn(primal_start)

    def over_col(x):
        return exchange(x, "col", n_col, sorted(range(1, n_col), key=lambda m: (m != 2, m)))

    def over_plane(chip, op=jnp.add):
        return tree(exchange(chip, "row", n_row, range(2, n_row, 2)), op)

    def other_core(x):
        return swap(x, "row", n_row, 1)

    def over_row(mine, theirs):
        summed = over_plane(mine + other_core(theirs))
        return summed, other_core(summed)

    xat = jnp.concatenate([constraint_cols.reshape(-1), factor_cols.reshape(-1)])
    xat = (xat + jnp.where(odd_core, half, 0)) % xcount
    yat = jnp.concatenate([constraint_rows.reshape(-1), ycount + factor_rows.reshape(-1)])
    part = jnp.arange(PARTS * count, dtype=jnp.int32) % PARTS

    def pick(at, size):
        place = part * size + jnp.repeat(at, PARTS)
        return (place[:, None] == jnp.arange(PARTS * size, dtype=jnp.int32)[None, :]).astype(BF16)

    gf = pick(xat, xcount)
    gb = pick(yat, full)
    columns = jnp.concatenate([xat[0::2], xat[1::2]])
    sb = (jnp.arange(xcount, dtype=jnp.int32)[:, None] == columns[None, :]).astype(BF16)
    at_rows = jnp.pad(yat.astype(F32), (0, 8 * width - count)).reshape(8, width)

    block = 16 if acount % 16 == 0 and fcount % 16 == 0 else 8
    a_steps, f_steps = acount // block, fcount // block
    matrix = pl.BlockSpec((block // 2, 2 * width, 2 * width), lambda i: (i, 0, 0))
    matrices = jax.ShapeDtypeStruct((pairs, 2 * width, 2 * width), BF16)
    tiles, turned, squares = pl.pallas_call(
        functools.partial(init_kernel, a_steps),
        grid=(a_steps + f_steps,),
        in_specs=[
            pl.BlockSpec((block, width, width), lambda i: (jnp.minimum(i, a_steps - 1), 0, 0)),
            pl.BlockSpec((block, width, width), lambda i: (jnp.maximum(i - a_steps, 0), 0, 0)),
        ],
        out_specs=(matrix, matrix, pl.BlockSpec((block, width), lambda i: (i, 0))),
        out_shape=(matrices, matrices, jax.ShapeDtypeStruct((count, width), F32)),
        compiler_params=pltpu.CompilerParams(vmem_limit_bytes=VMEM_LIMIT),
        name="split_tiles",
    )(pltpu.with_memory_space_constraint(ctiles, pltpu.HBM), pltpu.with_memory_space_constraint(ftiles, pltpu.HBM))

    scratch = (
        pltpu.VMEM((PARTS * count, 2 * width), BF16),
        pltpu.VMEM((PARTS * count, width), F32),
        pltpu.VMEM((PARTS * count, width), F32),
    )
    xs, ys, small = (xcount, width), (full, width), (8, width)
    sent, summed = (count + 8, width), (half + 8, width)

    (parts,) = call(first_forward_kernel, "first_forward", [sent], (primal_start, at_rows, gf, turned), scratch)
    mine, theirs, y0, s_all = call(
        functools.partial(first_backward_kernel, n_col, ycount, acount),
        "first_backward",
        [xs, xs, ys, jax.ShapeDtypeStruct((n_col, full, count), BF16)],
        (rho, *over_col(parts), gb, sb, tiles, squares, slack_start, dual_start),
        scratch,
        scalar=True,
    )
    resid, u, precond, parts = call(
        second_forward_kernel,
        "second_forward",
        [xs, xs, xs, sent],
        (*over_row(mine, theirs), primal_start, diag_cost, linear_cost, gf, turned),
        scratch,
    )
    v, yv = primal_start, y0
    p = yp = sc = alpha = None
    for step in range(CG):
        first, last = step == 0, step + 1 == CG
        state = (yv,) if first else (yp, yv, sc, alpha)
        mats = () if last else (gb, sb, tiles)
        *z, yp, yv, sc = call(
            functools.partial(backward_kernel, n_col, ycount, first, last),
            "last_norm" if last else "backward",
            ([small] if last else [summed, summed]) + [ys, ys, small],
            (rho, *over_col(parts), s_all, *state, *mats),
            () if last else scratch,
            scalar=True,
        )
        if last:
            break
        p, v, resid, u, alpha, parts = call(
            functools.partial(forward_kernel, first),
            "forward",
            [xs, xs, xs, xs, small, sent],
            (*over_row(*z), *(() if first else (p,)), u, v, resid, diag_cost, precond, sc, gf, turned),
            scratch,
        )
    norm = over_plane(z[0] + other_core(z[0]))
    primal_next, slack_next, dual_next, mine, theirs = call(
        functools.partial(final_kernel, ycount),
        "final",
        [xs, (ycount, width), (ycount, width), summed, summed],
        (rho, norm, u, p, v, primal_start, sc, yp, yv, y0)
        + (slack_start, dual_start, lower_bound, upper_bound, gb, sb, tiles),
        scratch,
        scalar=True,
    )

    def join(a, b):
        is_sum = lax.broadcasted_iota(jnp.int32, a.shape, 0) < half
        return jnp.where(is_sum, a + b, jnp.maximum(a, b))

    z = over_plane(join(mine, other_core(theirs)), join)
    (worst,) = call(residual_kernel, "residuals", [small], (z, primal_next, diag_cost, linear_cost))
    worst = jnp.maximum(worst, other_core(worst))
    worst = tree(over_col(worst), jnp.maximum)
    return (turn(primal_next), slack_next, dual_next, jnp.max(worst[:4]), jnp.max(worst[4:]))


def solution(mesh):
    placed = (
        P("row", "col", None, None),
        P("row", "col"),
        P("row", "col"),
        P("row", "col", None, None),
        P("row", "col"),
        P("row", "col"),
        P("col", None),
        P("col", None),
        P("row", None),
        P("row", None),
        P("col", None),
        P("row", None),
        P("row", None),
        P(),
    )
    return jax.shard_map(
        functools.partial(local, mesh.shape["row"], mesh.shape["col"]),
        mesh=mesh,
        in_specs=placed,
        out_specs=(P("col", None), P("row", None), P("row", None), P(), P()),
        check_vma=False,
    )
```

```python
import functools

import jax
import jax.numpy as jnp
from jax import lax
from jax.experimental import pallas as pl
from jax.experimental.pallas import tpu as pltpu
from jax.sharding import PartitionSpec as P

YG = 64
CG = 6

SIGMA = 1e-06
RELAX = 1.6

F32 = jnp.float32
BF16 = jnp.bfloat16
LANES = 128
UNROLL = 6
LANES = 128
TILES = 8
VMEM_LIMIT = 24 * 1024 * 1024


def dot(a, b):
    return lax.dot_general(a, b, (((1,), (0,)), ((), ())), preferred_element_type=F32)


def split2(x):
    high = x.astype(BF16)
    return high, (x - high.astype(F32)).astype(BF16)


def split3(x):
    high = x.astype(BF16)
    return (high, *split2(x - high.astype(F32)))


def tree(parts, op=jnp.add):
    parts = list(parts)
    while len(parts) > 1:
        parts = [op(parts[i], parts[i + 1]) for i in range(0, len(parts), 2)]
    return parts[0]


def row_sum(x):
    return jnp.sum(x, axis=0, keepdims=True)


def half_sum(x):
    half = x.shape[0] // 2
    return row_sum(x[:half]) + row_sum(x[half:])


def turn(odd, x):
    half = x.shape[0] // 2
    return jnp.where(odd, jnp.concatenate([x[half:], x[:half]], axis=0), x)


def pad_rows(rows):
    return jnp.concatenate(list(rows) + [jnp.zeros((8 - len(rows), LANES), F32)], axis=0)


def gather(onehot_ref, x):
    both = dot(onehot_ref[...], jnp.concatenate(split2(x), axis=1))
    high, low = both[:, :LANES], both[:, LANES:]
    blocks = high.shape[0] // TILES
    shape = (blocks, TILES, LANES)
    return jnp.concatenate([high.reshape(shape), low.reshape(shape)], axis=1).reshape(2 * TILES * blocks, LANES)


def scatter(onehot, x):
    both = dot(onehot, jnp.concatenate(split2(x), axis=1))
    return both[:, :LANES] + both[:, LANES:]


def run_tiles(w_ref, l_ref, finish):
    pairs = TILES // 2
    blocks = w_ref.shape[0] // pairs
    unroll = next(n for n in (UNROLL, 6, 4, 3, 2, 1) if blocks % n == 0)
    of_pair = lax.broadcasted_iota(jnp.int32, (2 * TILES, 2 * LANES), 0) % TILES // 2

    def body(step, carry):
        for inner in range(unroll):
            block = step * unroll + inner
            left = l_ref[pl.ds(pl.multiple_of(block * 2 * TILES, 2 * TILES), 2 * TILES), :]
            out = dot(left, w_ref[pairs * block])
            for k in range(1, pairs):
                out = jnp.where(of_pair == k, dot(left, w_ref[pairs * block + k]), out)
            finish(pl.multiple_of(block * TILES, TILES), out[:TILES] + out[TILES:])
        return carry

    lax.fori_loop(0, blocks // unroll, body, 0)


def forward_parts(vec, gf_ref, wt_ref, out_ref, l_ref):
    picked = gather(gf_ref, vec)
    first = lax.broadcasted_iota(jnp.int32, picked.shape, 0) % 2 == 0
    zero = jnp.zeros_like(picked)
    l_ref[:, :LANES] = jnp.where(first, picked, zero).astype(BF16)
    l_ref[:, LANES:] = jnp.where(first, zero, picked).astype(BF16)

    def finish(at, out):
        out_ref[pl.ds(at, TILES), :] = out[:, :LANES] + out[:, LANES:]

    run_tiles(wt_ref, l_ref, finish)


def backward_sum(vec, gb_ref, sb_ref, w_ref, l_ref, rows_ref):
    picked = gather(gb_ref, vec).astype(BF16)
    l_ref[:, :LANES] = picked
    l_ref[:, LANES:] = picked
    first = lax.broadcasted_iota(jnp.int32, (TILES, LANES), 0) % 2 == 0

    def finish(at, out):
        rows_ref[pl.ds(at, TILES), :] = jnp.where(first, out[:, :LANES], out[:, LANES:])

    run_tiles(w_ref, l_ref, finish)
    return scatter(sb_ref[...], rows_ref[...])


def gathered_rows(part_refs, s_ref):
    count = s_ref.shape[2]
    return tree(scatter(s_ref[j], ref[:count, :]) for j, ref in enumerate(part_refs))


def put_halves(refs, total, extra):
    half = total.shape[0] // 2
    for ref, part in zip(refs, (total[:half], total[half:])):
        ref[:half, :] = part
        ref[half:, :] = extra


def select_columns(ref, rows):
    size, count = ref.shape
    for row in range(pl.cdiv(count, LANES)):
        width = min(LANES, count - row * LANES)
        hit = lax.broadcasted_iota(jnp.int32, (size, width), 0) == rows[row : row + 1, :width].astype(jnp.int32)
        ref[:, row * LANES : row * LANES + width] = jnp.where(hit, 1.0, 0.0).astype(BF16)


def select_rows(ref, rows):
    count, size = ref.shape
    across = rows.T.astype(jnp.int32)
    for row in range(pl.cdiv(count, LANES)):
        width = min(LANES, count - row * LANES)
        hit = lax.broadcasted_iota(jnp.int32, (width, size), 1) == across[:width, row : row + 1]
        ref[row * LANES : row * LANES + width, :] = jnp.where(hit, 1.0, 0.0).astype(BF16)


def both_kinds(a_steps, a_ref, g_ref, convert):
    step = pl.program_id(0)

    @pl.when(step < a_steps)
    def _():
        convert(a_ref)

    @pl.when(step >= a_steps)
    def _():
        convert(g_ref)


def split_transposed_kernel(a_steps, rho_ref, a_ref, g_ref, wt_ref):
    def convert(ref):
        for t in range(ref.shape[0]):
            at = (t % 2) * LANES
            high, low = split2(ref[t].T)
            wt_ref[t // 2, at : at + LANES, :LANES] = high
            wt_ref[t // 2, at : at + LANES, LANES:] = low

    both_kinds(a_steps, a_ref, g_ref, convert)


def split_kernel(a_steps, rho_ref, a_ref, g_ref, w_ref, sq_ref):
    def convert(ref):
        for t in range(ref.shape[0]):
            at = (t % 2) * LANES
            tile = ref[t]
            high, low = split2(tile)
            w_ref[t // 2, :LANES, at : at + LANES] = high
            w_ref[t // 2, LANES:, at : at + LANES] = low
            sq_ref[t : t + 1, :] = row_sum(tile * tile)

    both_kinds(a_steps, a_ref, g_ref, convert)


def turned_places(odd, places, xcount):
    half = xcount // 2
    moved = jnp.where(places >= half, places - half, places + half)
    return jnp.where(odd, moved, places)


def first_forward_kernel(odd_ref, v_in_ref, at_ref, wt_ref, out_ref, v_ref, gf_ref, l_ref):
    odd = odd_ref[0] == 1
    count = 2 * wt_ref.shape[0]
    v = turn(odd, v_in_ref[...])
    v_ref[...] = v
    out_ref[count:, :] = at_ref[...]
    xrows = jnp.concatenate([at_ref[4:], at_ref[:4]], axis=0)
    select_rows(gf_ref, turned_places(odd, xrows, v.shape[0]))
    forward_parts(v, gf_ref, wt_ref, out_ref, l_ref)


def first_backward_kernel(n_col, ycount, acount, *refs):
    rho_ref, odd_ref, *refs = refs
    part_refs, refs = refs[:n_col], refs[n_col:]
    (w_ref, sq_ref, slack_ref, dual_ref), refs = refs[:4], refs[4:]
    mine_ref, theirs_ref, y_ref, s_ref, gb_ref, sb_ref, l_ref, rows_ref = refs
    rho, odd = rho_ref[0], odd_ref[0] == 1
    count = s_ref.shape[2]
    for j, ref in enumerate(part_refs):
        select_columns(s_ref.at[j], ref[count:, :])
    places = part_refs[0][count:, :]
    select_rows(gb_ref, places)
    select_columns(sb_ref, turned_places(odd, places[4:], sb_ref.shape[0]))
    full = gathered_rows(part_refs, s_ref)
    y_ref[...] = full
    top = rho * slack_ref[...] - dual_ref[...] - rho * full[:ycount]
    vec = jnp.concatenate([top, -full[ycount:]], axis=0)
    total = backward_sum(vec, gb_ref, sb_ref, w_ref, l_ref, rows_ref)
    squares = sq_ref[...]
    is_a = lax.broadcasted_iota(jnp.int32, squares.shape, 0) < acount
    parts = split3(jnp.where(is_a, rho * squares, squares))
    squares = sum(dot(sb_ref[...], part) for part in parts)
    half = total.shape[0] // 2
    mine_ref[:half, :] = total[:half]
    mine_ref[half:, :] = squares[:half]
    theirs_ref[:half, :] = total[half:]
    theirs_ref[half:, :] = squares[half:]


def finish_forward(u, p, resid, shifted, out_ref, gf_ref, w_ref, l_ref):
    count = 2 * w_ref.shape[0]
    weighted = shifted * u
    rows = [half_sum(resid * u), half_sum(weighted * u)]
    if p is not None:
        rows.append(half_sum(weighted * p))
    out_ref[count:, :] = pad_rows(rows)
    forward_parts(u, gf_ref, w_ref, out_ref, l_ref)


def second_forward_kernel(odd_ref, mine_ref, theirs_ref, v_ref, d_in_ref, c_in_ref, gf_ref, w_ref, *refs):
    r_ref, u_ref, pre_ref, d_ref, c_ref, out_ref, l_ref = refs
    odd = odd_ref[0] == 1
    half = v_ref.shape[0] // 2
    total = jnp.concatenate([mine_ref[:half, :], theirs_ref[:half, :]], axis=0)
    squares = jnp.concatenate([mine_ref[half:, :], theirs_ref[half:, :]], axis=0)
    v, d, c = v_ref[...], turn(odd, d_in_ref[...]), turn(odd, c_in_ref[...])
    d_ref[...] = d
    c_ref[...] = c
    resid = total - c - d * v
    shifted = d + SIGMA
    pre = shifted + squares
    u = resid / pre
    r_ref[...] = resid
    u_ref[...] = u
    pre_ref[...] = pre
    finish_forward(u, None, resid, shifted, out_ref, gf_ref, w_ref, l_ref)


def step_scalars(first, part_refs, sc_old_ref, count):
    totals = jnp.sum(tree(ref[count:, :] for ref in part_refs), axis=1, keepdims=True)
    gamma, one, two = totals[0:1], totals[1:2], totals[2:3]
    if first:
        return gamma, jnp.zeros_like(gamma), one
    old = sc_old_ref[...]
    beta = gamma / old[0:1, 0:1]
    return gamma, beta, one + beta * (2.0 * two + beta * old[2:3, 0:1])


def wide(x):
    return jnp.broadcast_to(x, (1, LANES))


def backward_kernel(n_col, ycount, first, last, *refs):
    rho_ref, *refs = refs
    part_refs, refs = refs[:n_col], refs[n_col:]
    s_ref, refs = refs[0], refs[1:]
    sc_old_ref = None
    if not first:
        (yp_old_ref, yv_old_ref, sc_old_ref, alpha_ref), refs = refs[:4], refs[4:]
    else:
        (yv_old_ref,), refs = refs[:1], refs[1:]
    if not last:
        (gb_ref, sb_ref, w_ref), refs = refs[:3], refs[3:]
    if last:
        z_ref, *refs = refs
    else:
        mine_ref, theirs_ref, *refs = refs
    yp_ref, yv_ref, sc_ref, *scratch = refs
    rho = rho_ref[0]
    full = gathered_rows(part_refs, s_ref)
    gamma, beta, pdp = step_scalars(first, part_refs, sc_old_ref, s_ref.shape[2])
    sc_ref[...] = pad_rows([wide(gamma), wide(beta), wide(pdp)])
    if first:
        yp = full
        yv_ref[...] = yv_old_ref[...]
    else:
        yp_old = yp_old_ref[...]
        yp = full + beta * yp_old
        yv_ref[...] = yv_old_ref[...] + alpha_ref[0:1, 0:1] * yp_old
    yp_ref[...] = yp
    scaled = jnp.concatenate([rho * yp[:ycount], yp[ycount:]], axis=0)
    norm = pad_rows([row_sum(scaled * yp)])
    if last:
        z_ref[...] = norm
    else:
        put_halves((mine_ref, theirs_ref), backward_sum(scaled, gb_ref, sb_ref, w_ref, *scratch), norm)


def step_alpha(extra, sc_ref):
    norm = jnp.sum(extra[0:1], axis=1, keepdims=True)
    return sc_ref[0:1, 0:1] / (sc_ref[2:3, 0:1] + norm)


def forward_kernel(first, *refs):
    (mine_ref, theirs_ref), refs = refs[:2], refs[2:]
    if not first:
        p_old_ref, refs = refs[0], refs[1:]
    (u_old_ref, v_old_ref, r_old_ref, d_ref, pre_ref, sc_ref, gf_ref, w_ref), refs = refs[:8], refs[8:]
    p_ref, v_ref, r_ref, u_ref, alpha_ref, out_ref, *scratch = refs
    half = d_ref.shape[0] // 2
    total = jnp.concatenate([mine_ref[:half, :], theirs_ref[:half, :]], axis=0)
    alpha = step_alpha(mine_ref[half:, :], sc_ref)
    p = u_old_ref[...]
    if not first:
        p = p + sc_ref[1:2, 0:1] * p_old_ref[...]
    shifted = d_ref[...] + SIGMA
    resid = r_old_ref[...] - alpha * (shifted * p + total)
    u = resid / pre_ref[...]
    p_ref[...] = p
    v_ref[...] = v_old_ref[...] + alpha * p
    r_ref[...] = resid
    u_ref[...] = u
    alpha_ref[...] = jnp.broadcast_to(alpha, (8, LANES))
    finish_forward(u, p, resid, shifted, out_ref, gf_ref, w_ref, *scratch)


def final_kernel(ycount, *refs):
    rho_ref, odd_ref, t_ref, *refs = refs
    (u_ref, p_old_ref, v_ref, start_ref, sc_ref, yp_ref, yv_ref, y0_ref), refs = refs[:8], refs[8:]
    (slack_ref, dual_ref, lower_ref, upper_ref, gb_ref, sb_ref, w_ref), refs = refs[:7], refs[7:]
    primal_out, half_out, slack_out, dual_out, mine_ref, theirs_ref, *scratch = refs
    rho = rho_ref[0]
    alpha = step_alpha(t_ref[...], sc_ref)
    p = u_ref[...] + sc_ref[1:2, 0:1] * p_old_ref[...]
    v = v_ref[...] + alpha * p
    primal = RELAX * v + (1.0 - RELAX) * start_ref[...]
    primal_out[...] = turn(odd_ref[0] == 1, primal)
    half_out[...] = primal[: primal.shape[0] // 2]
    image = yv_ref[...] + alpha * yp_ref[...]
    image_next = RELAX * image + (1.0 - RELAX) * y0_ref[...]
    dual = dual_ref[...]
    relaxed = RELAX * image[:ycount] + (1.0 - RELAX) * slack_ref[...]
    slack_next = jnp.minimum(jnp.maximum(relaxed + dual / rho, lower_ref[...]), upper_ref[...])
    dual_next = dual + rho * (relaxed - slack_next)
    slack_out[...] = slack_next
    dual_out[...] = dual_next
    worst = jnp.max(jnp.abs(image_next[:ycount] - slack_next), axis=0, keepdims=True)
    vec = jnp.concatenate([dual_next, image_next[ycount:]], axis=0)
    total = backward_sum(vec, gb_ref, sb_ref, w_ref, *scratch)
    put_halves((mine_ref, theirs_ref), total, jnp.broadcast_to(worst, (8, LANES)))


def residual_kernel(z_ref, primal_ref, d_ref, c_ref, out_ref):
    half = d_ref.shape[0] // 2
    dvec = d_ref[:half, :] * primal_ref[...] + z_ref[:half, :] + c_ref[:half, :]
    worst = jnp.max(jnp.abs(dvec), axis=0, keepdims=True)
    out_ref[...] = jnp.concatenate([z_ref[half : half + 4, :], jnp.broadcast_to(worst, (4, LANES))], axis=0)


VMEM_SPEC = pl.BlockSpec(memory_space=pltpu.VMEM)
SMEM_SPEC = pl.BlockSpec(memory_space=pltpu.SMEM)


def call(kernel, name, outs, args, scratch=(), scalars=0):
    specs = [SMEM_SPEC if i < scalars else VMEM_SPEC for i in range(len(args))]
    shapes = tuple(s if isinstance(s, jax.ShapeDtypeStruct) else jax.ShapeDtypeStruct(s, F32) for s in outs)
    return pl.pallas_call(
        kernel,
        out_shape=shapes,
        in_specs=specs,
        out_specs=tuple(VMEM_SPEC for _ in outs),
        scratch_shapes=list(scratch),
        compiler_params=pltpu.CompilerParams(vmem_limit_bytes=VMEM_LIMIT),
        name=name,
    )(*args)


def swap(x, axis, size, distance):
    return lax.ppermute(x, axis, [(i, i ^ distance) for i in range(size)])


def exchange(x, axis, size, distances):
    return [x] + [swap(x, axis, size, m) for m in distances]


def local(n_row, n_col, *args):
    (
        constraint_tiles,
        constraint_rows,
        constraint_cols,
        factor_tiles,
        factor_rows,
        factor_cols,
        diag_cost,
        linear_cost,
        lower_bound,
        upper_bound,
        primal_start,
        slack_start,
        dual_start,
        penalty,
    ) = args
    width = constraint_tiles.shape[2]
    ctiles = constraint_tiles.reshape(-1, width, width)
    ftiles = factor_tiles.reshape(-1, width, width)
    acount, fcount = ctiles.shape[0], ftiles.shape[0]
    count = acount + fcount
    pairs = count // 2
    xcount = primal_start.shape[0]
    ycount = slack_start.shape[0]
    full = ycount + YG
    half = xcount // 2

    def over_col(x):
        return exchange(x, "col", n_col, sorted(range(1, n_col), key=lambda m: (m != 2, m)))

    def over_plane(chip, op=jnp.add):
        return tree(exchange(chip, "row", n_row, range(2, n_row, 2)), op)

    def other_core(x):
        return swap(x, "row", n_row, 1)

    def over_row(mine, theirs):
        summed = over_plane(mine + other_core(theirs))
        return summed, other_core(summed)

    def places(a, f):
        at = jnp.concatenate([a.reshape(-1), f.reshape(-1)]).astype(F32)
        return jnp.pad(at, (0, 4 * width - count)).reshape(4, width)

    at = jnp.concatenate(
        [places(constraint_rows, factor_rows + ycount), places(constraint_cols, factor_cols)], axis=0
    )
    odd = (lax.axis_index("row") % 2).astype(jnp.int32).reshape(1)
    rho = penalty.reshape(1)
    at, odd, rho, ctiles, ftiles = lax.optimization_barrier((at, odd, rho, ctiles, ftiles))

    block = 16 if acount % 16 == 0 and fcount % 16 == 0 else 8
    a_steps, f_steps = acount // block, fcount // block
    matrix = pl.BlockSpec((block // 2, 2 * width, 2 * width), lambda i: (i, 0, 0))
    matrices = jax.ShapeDtypeStruct((pairs, 2 * width, 2 * width), BF16)

    def split_tiles(kernel, name, out_specs, out_shape, ctiles, ftiles):
        return pl.pallas_call(
            functools.partial(kernel, a_steps),
            grid=(a_steps + f_steps,),
            in_specs=[
                SMEM_SPEC,
                pl.BlockSpec((block, width, width), lambda i: (jnp.minimum(i, a_steps - 1), 0, 0)),
                pl.BlockSpec((block, width, width), lambda i: (jnp.maximum(i - a_steps, 0), 0, 0)),
            ],
            out_specs=out_specs,
            out_shape=out_shape,
            compiler_params=pltpu.CompilerParams(vmem_limit_bytes=VMEM_LIMIT),
            cost_estimate=pl.CostEstimate(
                flops=8 * count * width * width, bytes_accessed=4 * count * width * width, transcendentals=0
            ),
            name=name,
        )(
            rho,
            pltpu.with_memory_space_constraint(ctiles, pltpu.HBM),
            pltpu.with_memory_space_constraint(ftiles, pltpu.HBM),
        )

    turned = split_tiles(split_transposed_kernel, "split_transposed", matrix, matrices, ctiles, ftiles)

    left = pltpu.VMEM((2 * count, 2 * width), BF16)
    rows = pltpu.VMEM((count, width), F32)
    xs, ys, small = (xcount, width), (full, width), (8, width)
    sent, summed = (count + 8, width), (half + 8, width)
    bits = functools.partial(jax.ShapeDtypeStruct, dtype=BF16)

    parts, start, gf = call(
        first_forward_kernel,
        "first_forward",
        [sent, xs, bits((count, xcount))],
        (odd, primal_start, at, turned),
        [left],
        scalars=1,
    )
    parts, ctiles, ftiles = lax.optimization_barrier((parts, ctiles, ftiles))
    all_parts = over_col(parts)
    tiles, squares = split_tiles(
        split_kernel,
        "split",
        (matrix, pl.BlockSpec((block, width), lambda i: (i, 0))),
        (matrices, jax.ShapeDtypeStruct((count, width), F32)),
        ctiles,
        ftiles,
    )
    mine, theirs, y0, s_all, gb, sb = call(
        functools.partial(first_backward_kernel, n_col, ycount, acount),
        "first_backward",
        [xs, xs, ys, bits((n_col, full, count)), bits((count, full)), bits((xcount, count))],
        (rho, odd, *all_parts, tiles, squares, slack_start, dual_start),
        [left, rows],
        scalars=2,
    )
    resid, u, precond, diag, linear, parts = call(
        second_forward_kernel,
        "second_forward",
        [xs, xs, xs, xs, xs, sent],
        (odd, *over_row(mine, theirs), start, diag_cost, linear_cost, gf, turned),
        [left],
        scalars=1,
    )
    v, yv = start, y0
    p = yp = sc = alpha = None
    for step in range(CG):
        first, last = step == 0, step + 1 == CG
        state = (yv,) if first else (yp, yv, sc, alpha)
        mats = () if last else (gb, sb, tiles)
        *z, yp, yv, sc = call(
            functools.partial(backward_kernel, n_col, ycount, first, last),
            "last_norm" if last else "backward",
            ([small] if last else [summed, summed]) + [ys, ys, small],
            (rho, *over_col(parts), s_all, *state, *mats),
            [] if last else [left, rows],
            scalars=1,
        )
        if last:
            break
        p, v, resid, u, alpha, parts = call(
            functools.partial(forward_kernel, first),
            "forward",
            [xs, xs, xs, xs, small, sent],
            (*over_row(*z), *(() if first else (p,)), u, v, resid, diag, precond, sc, gf, turned),
            [left],
        )
    norm = over_plane(z[0] + other_core(z[0]))
    primal_next, primal_half, slack_next, dual_next, mine, theirs = call(
        functools.partial(final_kernel, ycount),
        "final",
        [xs, (half, width), (ycount, width), (ycount, width), summed, summed],
        (rho, odd, norm, u, p, v, start, sc, yp, yv, y0)
        + (slack_start, dual_start, lower_bound, upper_bound, gb, sb, tiles),
        [left, rows],
        scalars=2,
    )

    def join(a, b):
        is_sum = lax.broadcasted_iota(jnp.int32, a.shape, 0) < half
        return jnp.where(is_sum, a + b, jnp.maximum(a, b))

    z = over_plane(join(mine, other_core(theirs)), join)
    (worst,) = call(residual_kernel, "residuals", [small], (z, primal_half, diag, linear))
    worst = jnp.maximum(worst, other_core(worst))
    worst = tree(over_col(worst), jnp.maximum)
    return (primal_next, slack_next, dual_next, jnp.max(worst[:4]), jnp.max(worst[4:]))


def solution(mesh):
    placed = (
        P("row", "col", None, None),
        P("row", "col"),
        P("row", "col"),
        P("row", "col", None, None),
        P("row", "col"),
        P("row", "col"),
        P("col", None),
        P("col", None),
        P("row", None),
        P("row", None),
        P("col", None),
        P("row", None),
        P("row", None),
        P(),
    )
    return jax.shard_map(
        functools.partial(local, mesh.shape["row"], mesh.shape["col"]),
        mesh=mesh,
        in_specs=placed,
        out_specs=(P("col", None), P("row", None), P("row", None), P(), P()),
        check_vma=False,
    )
```

```python
import functools

import jax
import jax.numpy as jnp
from jax import lax
from jax.experimental import pallas as pl
from jax.experimental.pallas import tpu as pltpu
from jax.sharding import PartitionSpec as P

YG = 64
CG = 6

SIGMA = 1e-06
RELAX = 1.6

F32 = jnp.float32
BF16 = jnp.bfloat16
LANES = 128
UNROLL = 6
LANES = 128
TILES = 8
VMEM_LIMIT = 24 * 1024 * 1024


def dot(a, b):
    return lax.dot_general(a, b, (((1,), (0,)), ((), ())), preferred_element_type=F32)


def split2(x):
    high = x.astype(BF16)
    return high, (x - high.astype(F32)).astype(BF16)


def split3(x):
    high = x.astype(BF16)
    return (high, *split2(x - high.astype(F32)))


def tree(parts, op=jnp.add):
    parts = list(parts)
    while len(parts) > 1:
        parts = [op(parts[i], parts[i + 1]) for i in range(0, len(parts), 2)]
    return parts[0]


def row_sum(x):
    return jnp.sum(x, axis=0, keepdims=True)


def half_sum(x):
    half = x.shape[0] // 2
    return row_sum(x[:half]) + row_sum(x[half:])


def turn(odd, x):
    half = x.shape[0] // 2
    return jnp.where(odd, jnp.concatenate([x[half:], x[:half]], axis=0), x)


def pad_rows(rows):
    return jnp.concatenate(list(rows) + [jnp.zeros((8 - len(rows), LANES), F32)], axis=0)


def gather(onehot_ref, x):
    both = dot(onehot_ref[...], jnp.concatenate(split2(x), axis=1))
    high, low = both[:, :LANES], both[:, LANES:]
    blocks = high.shape[0] // TILES
    shape = (blocks, TILES, LANES)
    return jnp.concatenate([high.reshape(shape), low.reshape(shape)], axis=1).reshape(2 * TILES * blocks, LANES)


def scatter(onehot, x):
    both = dot(onehot, jnp.concatenate(split2(x), axis=1))
    return both[:, :LANES] + both[:, LANES:]


def one_block(w_ref, l_ref, block, finish):
    pairs = TILES // 2
    of_pair = lax.broadcasted_iota(jnp.int32, (2 * TILES, 2 * LANES), 0) % TILES // 2
    left = l_ref[pl.ds(pl.multiple_of(block * 2 * TILES, 2 * TILES), 2 * TILES), :]
    out = dot(left, w_ref[pairs * block])
    for k in range(1, pairs):
        out = jnp.where(of_pair == k, dot(left, w_ref[pairs * block + k]), out)
    finish(pl.multiple_of(block * TILES, TILES), out[:TILES] + out[TILES:])


def run_tiles(w_ref, l_ref, finish):
    blocks = w_ref.shape[0] // (TILES // 2)
    unroll = next(n for n in (UNROLL, 6, 4, 3, 2, 1) if blocks % n == 0)

    def body(step, carry):
        for inner in range(unroll):
            one_block(w_ref, l_ref, step * unroll + inner, finish)
        return carry

    lax.fori_loop(0, blocks // unroll, body, 0)


def forward_left(vec, gf_ref, l_ref):
    picked = gather(gf_ref, vec)
    first = lax.broadcasted_iota(jnp.int32, picked.shape, 0) % 2 == 0
    zero = jnp.zeros_like(picked)
    l_ref[:, :LANES] = jnp.where(first, picked, zero).astype(BF16)
    l_ref[:, LANES:] = jnp.where(first, zero, picked).astype(BF16)


def forward_finish(out_ref):
    def finish(at, out):
        out_ref[pl.ds(at, TILES), :] = out[:, :LANES] + out[:, LANES:]

    return finish


def forward_parts(vec, gf_ref, wt_ref, out_ref, l_ref):
    forward_left(vec, gf_ref, l_ref)
    run_tiles(wt_ref, l_ref, forward_finish(out_ref))


def backward_sum(vec, gb_ref, sb_ref, w_ref, l_ref, rows_ref):
    picked = gather(gb_ref, vec).astype(BF16)
    l_ref[:, :LANES] = picked
    l_ref[:, LANES:] = picked
    first = lax.broadcasted_iota(jnp.int32, (TILES, LANES), 0) % 2 == 0

    def finish(at, out):
        rows_ref[pl.ds(at, TILES), :] = jnp.where(first, out[:, :LANES], out[:, LANES:])

    run_tiles(w_ref, l_ref, finish)
    return scatter(sb_ref[...], rows_ref[...])


def gathered_rows(part_refs, s_ref):
    count = s_ref.shape[2]
    return tree(scatter(s_ref[j], ref[:count, :]) for j, ref in enumerate(part_refs))


def put_halves(refs, total, extra):
    half = total.shape[0] // 2
    for ref, part in zip(refs, (total[:half], total[half:])):
        ref[:half, :] = part
        ref[half:, :] = extra


def select_columns(ref, rows):
    size, count = ref.shape
    for row in range(pl.cdiv(count, LANES)):
        width = min(LANES, count - row * LANES)
        hit = lax.broadcasted_iota(jnp.int32, (size, width), 0) == rows[row : row + 1, :width].astype(jnp.int32)
        ref[:, row * LANES : row * LANES + width] = jnp.where(hit, 1.0, 0.0).astype(BF16)


def select_rows(ref, rows):
    count, size = ref.shape
    across = rows.T.astype(jnp.int32)
    for row in range(pl.cdiv(count, LANES)):
        width = min(LANES, count - row * LANES)
        hit = lax.broadcasted_iota(jnp.int32, (width, size), 1) == across[:width, row : row + 1]
        ref[row * LANES : row * LANES + width, :] = jnp.where(hit, 1.0, 0.0).astype(BF16)


def tile_copies(chunk, refs, held_ref, sems):
    copies, at = [], 0
    for ref in refs:
        for start in range(0, ref.shape[0], chunk):
            copies.append(
                pltpu.make_async_copy(
                    ref.at[pl.ds(start, chunk)], held_ref.at[pl.ds(at, chunk)], sems.at[len(copies)]
                )
            )
            at += chunk
    return copies


def wait_chunk(step, chunk, a_ref, held_ref, sems):
    at = pl.multiple_of(step * chunk, chunk)
    pltpu.make_async_copy(a_ref.at[pl.ds(0, chunk)], held_ref.at[pl.ds(at, chunk)], sems.at[step]).wait()


def odd_core():
    return lax.axis_index("row") % 2 == 1


def split_kernel(chunk, a_ref, g_ref, w_ref, sq_ref, held_ref, sems):
    copies = tile_copies(chunk, (a_ref, g_ref), held_ref, sems)
    for copy in copies:
        copy.start()

    def body(step, carry):
        wait_chunk(step, chunk, a_ref, held_ref, sems)
        for t in range(chunk):
            tile = held_ref[step * chunk + t]
            pair, at = (step * chunk + t) // 2, (t % 2) * LANES
            high, low = split2(tile)
            w_ref[pair, :LANES, at : at + LANES] = high
            w_ref[pair, LANES:, at : at + LANES] = low
            sq_ref[pl.ds(step * chunk + t, 1), :] = row_sum(tile * tile)
        return carry

    lax.fori_loop(0, len(copies), body, 0)


def turned_places(odd, places, xcount):
    half = xcount // 2
    moved = jnp.where(places >= half, places - half, places + half)
    return jnp.where(odd, moved, places)


def joined(at_ref, a_ref, f_ref, base=0):
    acount, fcount = a_ref.shape[1], f_ref.shape[1]
    at_ref[...] = jnp.zeros_like(at_ref)
    at_ref[0:1, :acount] = a_ref[...].astype(F32)
    at_ref[1:2, :fcount] = (f_ref[...] + base).astype(F32)
    a, f = at_ref[0:1, :], at_ref[1:2, :]
    moved = pltpu.roll(jnp.broadcast_to(f, (8, LANES)), acount % LANES, 1)[0:1]
    lane = lax.broadcasted_iota(jnp.int32, (1, LANES), 1)
    return [jnp.where(lane < acount, a, moved), moved]


def first_forward_kernel(chunk, ycount, rho_ref, *refs):
    (a_ref, g_ref), small_refs, refs = refs[:2], refs[2:7], refs[7:]
    (wt_ref, out_ref, v_ref, gf_ref, l_ref, at_ref), refs = refs[:6], refs[6:]
    small_held, (small_sems, held_ref, sems) = refs[:5], refs[5:]
    fetched = [pltpu.make_async_copy(a, b, small_sems.at[i]) for i, (a, b) in enumerate(zip(small_refs, small_held))]
    copies = tile_copies(chunk, (a_ref, g_ref), held_ref, sems)
    for copy in fetched + copies:
        copy.start()
    odd = odd_core()
    for copy in fetched:
        copy.wait()
    v_in_ref, arow_ref, acol_ref, frow_ref, fcol_ref = small_held
    count = 2 * wt_ref.shape[0]
    v = turn(odd, v_in_ref[...])
    v_ref[...] = v
    zero = [jnp.zeros((1, LANES), F32)] * 2
    yrows = joined(at_ref, arow_ref, frow_ref, ycount) + zero
    xrows = joined(at_ref, acol_ref, fcol_ref) + zero
    out_ref[count:, :] = jnp.concatenate(yrows + xrows, axis=0)
    places = jnp.concatenate(xrows + yrows, axis=0)
    select_rows(gf_ref, turned_places(odd, places, v.shape[0]))
    forward_left(v, gf_ref, l_ref)
    finish = forward_finish(out_ref)
    blocks = chunk // TILES

    def products(step):
        for inner in range(blocks):
            one_block(wt_ref, l_ref, step * blocks + inner, finish)

    def split(step):
        wait_chunk(step, chunk, a_ref, held_ref, sems)
        for t in range(chunk):
            pair, at = (step * chunk + t) // 2, (t % 2) * LANES
            high, low = split2(held_ref[step * chunk + t].T)
            wt_ref[pair, at : at + LANES, :LANES] = high
            wt_ref[pair, at : at + LANES, LANES:] = low

    split(0)

    def body(step, carry):
        products(step - 1)
        split(step)
        return carry

    lax.fori_loop(1, len(copies), body, 0)
    products(len(copies) - 1)


def first_backward_kernel(n_col, ycount, acount, *refs):
    rho_ref, *refs = refs
    part_refs, refs = refs[:n_col], refs[n_col:]
    (w_ref, sq_ref, slack_ref, dual_ref), refs = refs[:4], refs[4:]
    mine_ref, theirs_ref, y_ref, s_ref, gb_ref, sb_ref, l_ref, rows_ref = refs
    rho, odd = rho_ref[0], odd_core()
    count = s_ref.shape[2]
    for j, ref in enumerate(part_refs):
        select_columns(s_ref.at[j], ref[count:, :])
    places = part_refs[0][count:, :]
    select_rows(gb_ref, places)
    select_columns(sb_ref, turned_places(odd, places[4:], sb_ref.shape[0]))
    full = gathered_rows(part_refs, s_ref)
    y_ref[...] = full
    top = rho * slack_ref[...] - dual_ref[...] - rho * full[:ycount]
    vec = jnp.concatenate([top, -full[ycount:]], axis=0)
    total = backward_sum(vec, gb_ref, sb_ref, w_ref, l_ref, rows_ref)
    squares = sq_ref[...]
    is_a = lax.broadcasted_iota(jnp.int32, squares.shape, 0) < acount
    parts = split3(jnp.where(is_a, rho * squares, squares))
    squares = sum(dot(sb_ref[...], part) for part in parts)
    half = total.shape[0] // 2
    mine_ref[:half, :] = total[:half]
    mine_ref[half:, :] = squares[:half]
    theirs_ref[:half, :] = total[half:]
    theirs_ref[half:, :] = squares[half:]


def finish_forward(u, p, resid, shifted, out_ref, gf_ref, w_ref, l_ref):
    count = 2 * w_ref.shape[0]
    weighted = shifted * u
    rows = [half_sum(resid * u), half_sum(weighted * u)]
    if p is not None:
        rows.append(half_sum(weighted * p))
    out_ref[count:, :] = pad_rows(rows)
    forward_parts(u, gf_ref, w_ref, out_ref, l_ref)


def second_forward_kernel(mine_ref, theirs_ref, v_ref, d_in_ref, c_in_ref, gf_ref, w_ref, *refs):
    r_ref, u_ref, pre_ref, d_ref, c_ref, out_ref, l_ref = refs
    odd = odd_core()
    half = v_ref.shape[0] // 2
    total = jnp.concatenate([mine_ref[:half, :], theirs_ref[:half, :]], axis=0)
    squares = jnp.concatenate([mine_ref[half:, :], theirs_ref[half:, :]], axis=0)
    v, d, c = v_ref[...], turn(odd, d_in_ref[...]), turn(odd, c_in_ref[...])
    d_ref[...] = d
    c_ref[...] = c
    resid = total - c - d * v
    shifted = d + SIGMA
    pre = shifted + squares
    u = resid / pre
    r_ref[...] = resid
    u_ref[...] = u
    pre_ref[...] = pre
    finish_forward(u, None, resid, shifted, out_ref, gf_ref, w_ref, l_ref)


def step_scalars(first, part_refs, sc_old_ref, count):
    totals = jnp.sum(tree(ref[count:, :] for ref in part_refs), axis=1, keepdims=True)
    gamma, one, two = totals[0:1], totals[1:2], totals[2:3]
    if first:
        return gamma, jnp.zeros_like(gamma), one
    old = sc_old_ref[...]
    beta = gamma / old[0:1, 0:1]
    return gamma, beta, one + beta * (2.0 * two + beta * old[2:3, 0:1])


def wide(x):
    return jnp.broadcast_to(x, (1, LANES))


def backward_kernel(n_col, ycount, first, last, *refs):
    rho_ref, *refs = refs
    part_refs, refs = refs[:n_col], refs[n_col:]
    s_ref, refs = refs[0], refs[1:]
    sc_old_ref = None
    if not first:
        (yp_old_ref, yv_old_ref, sc_old_ref, alpha_ref), refs = refs[:4], refs[4:]
    else:
        (yv_old_ref,), refs = refs[:1], refs[1:]
    if not last:
        (gb_ref, sb_ref, w_ref), refs = refs[:3], refs[3:]
    if last:
        z_ref, *refs = refs
    else:
        mine_ref, theirs_ref, *refs = refs
    yp_ref, yv_ref, sc_ref, *scratch = refs
    rho = rho_ref[0]
    full = gathered_rows(part_refs, s_ref)
    gamma, beta, pdp = step_scalars(first, part_refs, sc_old_ref, s_ref.shape[2])
    sc_ref[...] = pad_rows([wide(gamma), wide(beta), wide(pdp)])
    if first:
        yp = full
        yv_ref[...] = yv_old_ref[...]
    else:
        yp_old = yp_old_ref[...]
        yp = full + beta * yp_old
        yv_ref[...] = yv_old_ref[...] + alpha_ref[0:1, 0:1] * yp_old
    yp_ref[...] = yp
    scaled = jnp.concatenate([rho * yp[:ycount], yp[ycount:]], axis=0)
    norm = pad_rows([row_sum(scaled * yp)])
    if last:
        z_ref[...] = norm
    else:
        put_halves((mine_ref, theirs_ref), backward_sum(scaled, gb_ref, sb_ref, w_ref, *scratch), norm)


def step_alpha(extra, sc_ref):
    norm = jnp.sum(extra[0:1], axis=1, keepdims=True)
    return sc_ref[0:1, 0:1] / (sc_ref[2:3, 0:1] + norm)


def forward_kernel(first, *refs):
    (mine_ref, theirs_ref), refs = refs[:2], refs[2:]
    if not first:
        p_old_ref, refs = refs[0], refs[1:]
    (u_old_ref, v_old_ref, r_old_ref, d_ref, pre_ref, sc_ref, gf_ref, w_ref), refs = refs[:8], refs[8:]
    p_ref, v_ref, r_ref, u_ref, alpha_ref, out_ref, *scratch = refs
    half = d_ref.shape[0] // 2
    total = jnp.concatenate([mine_ref[:half, :], theirs_ref[:half, :]], axis=0)
    alpha = step_alpha(mine_ref[half:, :], sc_ref)
    p = u_old_ref[...]
    if not first:
        p = p + sc_ref[1:2, 0:1] * p_old_ref[...]
    shifted = d_ref[...] + SIGMA
    resid = r_old_ref[...] - alpha * (shifted * p + total)
    u = resid / pre_ref[...]
    p_ref[...] = p
    v_ref[...] = v_old_ref[...] + alpha * p
    r_ref[...] = resid
    u_ref[...] = u
    alpha_ref[...] = jnp.broadcast_to(alpha, (8, LANES))
    finish_forward(u, p, resid, shifted, out_ref, gf_ref, w_ref, *scratch)


def final_kernel(ycount, *refs):
    rho_ref, t_ref, *refs = refs
    (u_ref, p_old_ref, v_ref, start_ref, sc_ref, yp_ref, yv_ref, y0_ref), refs = refs[:8], refs[8:]
    (slack_ref, dual_ref, lower_ref, upper_ref, gb_ref, sb_ref, w_ref), refs = refs[:7], refs[7:]
    primal_out, half_out, slack_out, dual_out, mine_ref, theirs_ref, *scratch = refs
    rho = rho_ref[0]
    alpha = step_alpha(t_ref[...], sc_ref)
    p = u_ref[...] + sc_ref[1:2, 0:1] * p_old_ref[...]
    v = v_ref[...] + alpha * p
    primal = RELAX * v + (1.0 - RELAX) * start_ref[...]
    primal_out[...] = turn(odd_core(), primal)
    half_out[...] = primal[: primal.shape[0] // 2]
    image = yv_ref[...] + alpha * yp_ref[...]
    image_next = RELAX * image + (1.0 - RELAX) * y0_ref[...]
    dual = dual_ref[...]
    relaxed = RELAX * image[:ycount] + (1.0 - RELAX) * slack_ref[...]
    slack_next = jnp.minimum(jnp.maximum(relaxed + dual / rho, lower_ref[...]), upper_ref[...])
    dual_next = dual + rho * (relaxed - slack_next)
    slack_out[...] = slack_next
    dual_out[...] = dual_next
    worst = jnp.max(jnp.abs(image_next[:ycount] - slack_next), axis=0, keepdims=True)
    vec = jnp.concatenate([dual_next, image_next[ycount:]], axis=0)
    total = backward_sum(vec, gb_ref, sb_ref, w_ref, *scratch)
    put_halves((mine_ref, theirs_ref), total, jnp.broadcast_to(worst, (8, LANES)))


def residual_kernel(z_ref, primal_ref, d_ref, c_ref, out_ref):
    half = d_ref.shape[0] // 2
    dvec = d_ref[:half, :] * primal_ref[...] + z_ref[:half, :] + c_ref[:half, :]
    worst = jnp.max(jnp.abs(dvec), axis=0, keepdims=True)
    out_ref[...] = jnp.concatenate([z_ref[half : half + 4, :], jnp.broadcast_to(worst, (4, LANES))], axis=0)


VMEM_SPEC = pl.BlockSpec(memory_space=pltpu.VMEM)
SMEM_SPEC = pl.BlockSpec(memory_space=pltpu.SMEM)
HBM_SPEC = pl.BlockSpec(memory_space=pltpu.HBM)


def call(kernel, name, outs, args, scratch=(), scalars=0, streamed=0, cost=None):
    kinds = [SMEM_SPEC] * scalars + [HBM_SPEC] * streamed
    specs = kinds + [VMEM_SPEC] * (len(args) - len(kinds))
    args = [
        pltpu.with_memory_space_constraint(x, pltpu.HBM) if scalars <= i < scalars + streamed else x
        for i, x in enumerate(args)
    ]
    shapes = tuple(s if isinstance(s, jax.ShapeDtypeStruct) else jax.ShapeDtypeStruct(s, F32) for s in outs)
    return pl.pallas_call(
        kernel,
        out_shape=shapes,
        in_specs=specs,
        out_specs=tuple(VMEM_SPEC for _ in outs),
        scratch_shapes=list(scratch),
        compiler_params=pltpu.CompilerParams(vmem_limit_bytes=VMEM_LIMIT),
        cost_estimate=cost,
        name=name,
    )(*args)


def swap(x, axis, size, distance):
    return lax.ppermute(x, axis, [(i, i ^ distance) for i in range(size)])


def exchange(x, axis, size, distances):
    return [x] + [swap(x, axis, size, m) for m in distances]


def local(n_row, n_col, *args):
    (
        constraint_tiles,
        constraint_rows,
        constraint_cols,
        factor_tiles,
        factor_rows,
        factor_cols,
        diag_cost,
        linear_cost,
        lower_bound,
        upper_bound,
        primal_start,
        slack_start,
        dual_start,
        penalty,
    ) = args
    width = constraint_tiles.shape[2]
    ctiles = constraint_tiles.reshape(-1, width, width)
    ftiles = factor_tiles.reshape(-1, width, width)
    acount, fcount = ctiles.shape[0], ftiles.shape[0]
    count = acount + fcount
    pairs = count // 2
    xcount = primal_start.shape[0]
    ycount = slack_start.shape[0]
    full = ycount + YG
    half = xcount // 2

    def over_col(x):
        return exchange(x, "col", n_col, sorted(range(1, n_col), key=lambda m: (m != 2, m)))

    def over_plane(chip, op=jnp.add):
        return tree(exchange(chip, "row", n_row, range(2, n_row, 2)), op)

    def other_core(x):
        return swap(x, "row", n_row, 1)

    def over_row(mine, theirs):
        summed = over_plane(mine + other_core(theirs))
        return summed, other_core(summed)

    rho = penalty.reshape(1)
    chunk = next(n for n in (16, 8) if acount % n == 0 and fcount % n == 0)
    assert acount <= width and fcount <= width
    matrices = jax.ShapeDtypeStruct((pairs, 2 * width, 2 * width), BF16)
    held = [
        pltpu.VMEM((count, width, width), F32),
        pltpu.SemaphoreType.DMA((count // chunk,)),
    ]

    left = pltpu.VMEM((2 * count, 2 * width), BF16)
    rows = pltpu.VMEM((count, width), F32)
    xs, ys, small = (xcount, width), (full, width), (8, width)
    sent, summed = (count + 8, width), (half + 8, width)
    bits = functools.partial(jax.ShapeDtypeStruct, dtype=BF16)

    turned, parts, start, gf = call(
        functools.partial(first_forward_kernel, chunk, ycount),
        "first_forward",
        [matrices, sent, xs, bits((count, xcount))],
        (rho, ctiles, ftiles, primal_start)
        + tuple(x.reshape(1, -1) for x in (constraint_rows, constraint_cols, factor_rows, factor_cols)),
        [left, pltpu.VMEM((8, width), F32), pltpu.VMEM(xs, F32)]
        + [pltpu.VMEM((1, n), jnp.int32) for n in (acount, acount, fcount, fcount)]
        + [pltpu.SemaphoreType.DMA((5,)), *held],
        scalars=1,
        streamed=7,
    )
    parts, ctiles, ftiles = lax.optimization_barrier((parts, ctiles, ftiles))
    all_parts = over_col(parts)
    tiles, squares = call(
        functools.partial(split_kernel, chunk),
        "split",
        [matrices, (count, width)],
        (ctiles, ftiles),
        held,
        streamed=2,
        cost=pl.CostEstimate(
            flops=8 * count * width * width, bytes_accessed=4 * count * width * width, transcendentals=0
        ),
    )
    mine, theirs, y0, s_all, gb, sb = call(
        functools.partial(first_backward_kernel, n_col, ycount, acount),
        "first_backward",
        [xs, xs, ys, bits((n_col, full, count)), bits((count, full)), bits((xcount, count))],
        (rho, *all_parts, tiles, squares, slack_start, dual_start),
        [left, rows],
        scalars=1,
    )
    resid, u, precond, diag, linear, parts = call(
        second_forward_kernel,
        "second_forward",
        [xs, xs, xs, xs, xs, sent],
        (*over_row(mine, theirs), start, diag_cost, linear_cost, gf, turned),
        [left],
    )
    v, yv = start, y0
    p = yp = sc = alpha = None
    for step in range(CG):
        first, last = step == 0, step + 1 == CG
        state = (yv,) if first else (yp, yv, sc, alpha)
        mats = () if last else (gb, sb, tiles)
        *z, yp, yv, sc = call(
            functools.partial(backward_kernel, n_col, ycount, first, last),
            "last_norm" if last else "backward",
            ([small] if last else [summed, summed]) + [ys, ys, small],
            (rho, *over_col(parts), s_all, *state, *mats),
            [] if last else [left, rows],
            scalars=1,
        )
        if last:
            break
        p, v, resid, u, alpha, parts = call(
            functools.partial(forward_kernel, first),
            "forward",
            [xs, xs, xs, xs, small, sent],
            (*over_row(*z), *(() if first else (p,)), u, v, resid, diag, precond, sc, gf, turned),
            [left],
        )
    norm = over_plane(z[0] + other_core(z[0]))
    primal_next, primal_half, slack_next, dual_next, mine, theirs = call(
        functools.partial(final_kernel, ycount),
        "final",
        [xs, (half, width), (ycount, width), (ycount, width), summed, summed],
        (rho, norm, u, p, v, start, sc, yp, yv, y0)
        + (slack_start, dual_start, lower_bound, upper_bound, gb, sb, tiles),
        [left, rows],
        scalars=1,
    )

    def join(a, b):
        is_sum = lax.broadcasted_iota(jnp.int32, a.shape, 0) < half
        return jnp.where(is_sum, a + b, jnp.maximum(a, b))

    z = over_plane(join(mine, other_core(theirs)), join)
    (worst,) = call(residual_kernel, "residuals", [small], (z, primal_half, diag, linear))
    worst = jnp.maximum(worst, other_core(worst))
    worst = tree(exchange(worst, "col", n_col, range(1, n_col)), jnp.maximum)
    return (primal_next, slack_next, dual_next, jnp.max(worst[:4]), jnp.max(worst[4:]))


def solution(mesh):
    placed = (
        P("row", "col", None, None),
        P("row", "col"),
        P("row", "col"),
        P("row", "col", None, None),
        P("row", "col"),
        P("row", "col"),
        P("col", None),
        P("col", None),
        P("row", None),
        P("row", None),
        P("col", None),
        P("row", None),
        P("row", None),
        P(),
    )
    return jax.shard_map(
        functools.partial(local, mesh.shape["row"], mesh.shape["col"]),
        mesh=mesh,
        in_specs=placed,
        out_specs=(P("col", None), P("row", None), P("row", None), P(), P()),
        check_vma=False,
    )
```

```python
import functools

import jax
import jax.numpy as jnp
from jax import lax
from jax.experimental import pallas as pl
from jax.experimental.pallas import tpu as pltpu
from jax.sharding import PartitionSpec as P

YG = 64
CG = 6

SIGMA = 1e-06
RELAX = 1.6

F32 = jnp.float32
BF16 = jnp.bfloat16
LANES = 128
UNROLL = 18
IN_FLIGHT = 2
LANES = 128
TILES = 8
VMEM_LIMIT = 24 * 1024 * 1024


def dot(a, b):
    return lax.dot_general(a, b, (((1,), (0,)), ((), ())), preferred_element_type=F32)


def split2(x):
    high = x.astype(BF16)
    return high, (x - high.astype(F32)).astype(BF16)


def split3(x):
    high = x.astype(BF16)
    return (high, *split2(x - high.astype(F32)))


def tree(parts, op=jnp.add):
    parts = list(parts)
    while len(parts) > 1:
        parts = [op(parts[i], parts[i + 1]) for i in range(0, len(parts), 2)]
    return parts[0]


def row_sum(x):
    return jnp.sum(x, axis=0, keepdims=True)


def half_sum(x):
    half = x.shape[0] // 2
    return row_sum(x[:half]) + row_sum(x[half:])


def turn(odd, x):
    half = x.shape[0] // 2
    return jnp.where(odd, jnp.concatenate([x[half:], x[:half]], axis=0), x)


def pad_rows(rows):
    return jnp.concatenate(list(rows) + [jnp.zeros((8 - len(rows), LANES), F32)], axis=0)


def gather(onehot_ref, x):
    both = dot(onehot_ref[...], jnp.concatenate(split2(x), axis=1))
    high, low = both[:, :LANES], both[:, LANES:]
    blocks = high.shape[0] // TILES
    shape = (blocks, TILES, LANES)
    return jnp.concatenate([high.reshape(shape), low.reshape(shape)], axis=1).reshape(2 * TILES * blocks, LANES)


def scatter(onehot, x):
    both = dot(onehot, jnp.concatenate(split2(x), axis=1))
    return both[:, :LANES] + both[:, LANES:]


def one_block(w_ref, l_ref, block, finish):
    pairs = TILES // 2
    of_pair = lax.broadcasted_iota(jnp.int32, (2 * TILES, 2 * LANES), 0) % TILES // 2
    left = l_ref[pl.ds(pl.multiple_of(block * 2 * TILES, 2 * TILES), 2 * TILES), :]
    out = dot(left, w_ref[pairs * block])
    for k in range(1, pairs):
        out = jnp.where(of_pair == k, dot(left, w_ref[pairs * block + k]), out)
    finish(pl.multiple_of(block * TILES, TILES), out[:TILES] + out[TILES:])


def run_tiles(w_ref, l_ref, most, finish):
    blocks = w_ref.shape[0] // (TILES // 2)
    unroll = next(n for n in (most, 6, 4, 3, 2, 1) if blocks % n == 0)

    def body(step, carry):
        for inner in range(unroll):
            one_block(w_ref, l_ref, step * unroll + inner, finish)
        return carry

    lax.fori_loop(0, blocks // unroll, body, 0)


def forward_left(vec, gf_ref, l_ref):
    picked = gather(gf_ref, vec)
    first = lax.broadcasted_iota(jnp.int32, picked.shape, 0) % 2 == 0
    zero = jnp.zeros_like(picked)
    l_ref[:, :LANES] = jnp.where(first, picked, zero).astype(BF16)
    l_ref[:, LANES:] = jnp.where(first, zero, picked).astype(BF16)


def forward_finish(out_ref):
    def finish(at, out):
        out_ref[pl.ds(at, TILES), :] = out[:, :LANES] + out[:, LANES:]

    return finish


def forward_parts(vec, gf_ref, wt_ref, out_ref, l_ref):
    forward_left(vec, gf_ref, l_ref)
    run_tiles(wt_ref, l_ref, UNROLL, forward_finish(out_ref))


def backward_sum(vec, gb_ref, sb_ref, w_ref, l_ref, rows_ref):
    picked = gather(gb_ref, vec).astype(BF16)
    l_ref[:, :LANES] = picked
    l_ref[:, LANES:] = picked
    first = lax.broadcasted_iota(jnp.int32, (TILES, LANES), 0) % 2 == 0

    def finish(at, out):
        rows_ref[pl.ds(at, TILES), :] = jnp.where(first, out[:, :LANES], out[:, LANES:])

    run_tiles(w_ref, l_ref, UNROLL, finish)
    return scatter(sb_ref[...], rows_ref[...])


def gathered_rows(part_refs, s_ref):
    count = s_ref.shape[2]
    return tree(scatter(s_ref[j], ref[:count, :]) for j, ref in enumerate(part_refs))


def put_halves(refs, total, extra):
    half = total.shape[0] // 2
    for ref, part in zip(refs, (total[:half], total[half:])):
        ref[:half, :] = part
        ref[half:, :] = extra


def select_columns(ref, rows):
    size, count = ref.shape
    for row in range(pl.cdiv(count, LANES)):
        width = min(LANES, count - row * LANES)
        hit = lax.broadcasted_iota(jnp.int32, (size, width), 0) == rows[row : row + 1, :width].astype(jnp.int32)
        ref[:, row * LANES : row * LANES + width] = jnp.where(hit, 1.0, 0.0).astype(BF16)


def select_rows(ref, rows):
    count, size = ref.shape
    across = rows.T.astype(jnp.int32)
    for row in range(pl.cdiv(count, LANES)):
        width = min(LANES, count - row * LANES)
        hit = lax.broadcasted_iota(jnp.int32, (width, size), 1) == across[:width, row : row + 1]
        ref[row * LANES : row * LANES + width, :] = jnp.where(hit, 1.0, 0.0).astype(BF16)


def tile_copies(chunk, refs, held_ref, sems):
    copies, at = [], 0
    for ref in refs:
        for start in range(0, ref.shape[0], chunk):
            copies.append(
                pltpu.make_async_copy(
                    ref.at[pl.ds(start, chunk)], held_ref.at[pl.ds(at, chunk)], sems.at[len(copies)]
                )
            )
            at += chunk
    return copies


def wait_chunk(step, chunk, copies, a_ref, held_ref, sems):
    for later in range(IN_FLIGHT, len(copies)):
        pl.when(step + IN_FLIGHT == later)(copies[later].start)
    at = pl.multiple_of(step * chunk, chunk)
    pltpu.make_async_copy(a_ref.at[pl.ds(0, chunk)], held_ref.at[pl.ds(at, chunk)], sems.at[step]).wait()


def odd_core():
    return lax.axis_index("row") % 2 == 1


def split_kernel(chunk, a_ref, g_ref, w_ref, sq_ref, held_ref, sems):
    copies = tile_copies(chunk, (a_ref, g_ref), held_ref, sems)
    for copy in copies:
        copy.start()

    def body(step, carry):
        wait_chunk(step, chunk, (), a_ref, held_ref, sems)
        for t in range(chunk):
            tile = held_ref[step * chunk + t]
            pair, at = (step * chunk + t) // 2, (t % 2) * LANES
            high, low = split2(tile)
            w_ref[pair, :LANES, at : at + LANES] = high
            w_ref[pair, LANES:, at : at + LANES] = low
            sq_ref[pl.ds(step * chunk + t, 1), :] = row_sum(tile * tile)
        return carry

    lax.fori_loop(0, len(copies), body, 0)


def turned_places(odd, places, xcount):
    half = xcount // 2
    moved = jnp.where(places >= half, places - half, places + half)
    return jnp.where(odd, moved, places)


def joined(at_ref, a_ref, f_ref, base=0):
    acount, fcount = a_ref.shape[1], f_ref.shape[1]
    at_ref[...] = jnp.zeros_like(at_ref)
    at_ref[0:1, :acount] = a_ref[...].astype(F32)
    at_ref[1:2, :fcount] = (f_ref[...] + base).astype(F32)
    a, f = at_ref[0:1, :], at_ref[1:2, :]
    moved = pltpu.roll(jnp.broadcast_to(f, (8, LANES)), acount % LANES, 1)[0:1]
    lane = lax.broadcasted_iota(jnp.int32, (1, LANES), 1)
    return [jnp.where(lane < acount, a, moved), moved]


def first_forward_kernel(chunk, ycount, rho_ref, *refs):
    (a_ref, g_ref), small_refs, refs = refs[:2], refs[2:7], refs[7:]
    (wt_ref, out_ref, v_ref, gf_ref, l_ref, at_ref), refs = refs[:6], refs[6:]
    small_held, (small_sems, held_ref, sems) = refs[:5], refs[5:]
    fetched = [pltpu.make_async_copy(a, b, small_sems.at[i]) for i, (a, b) in enumerate(zip(small_refs, small_held))]
    copies = tile_copies(chunk, (a_ref, g_ref), held_ref, sems)
    for copy in fetched + copies[:IN_FLIGHT]:
        copy.start()
    odd = odd_core()
    for copy in fetched:
        copy.wait()
    v_in_ref, arow_ref, acol_ref, frow_ref, fcol_ref = small_held
    count = 2 * wt_ref.shape[0]
    v = turn(odd, v_in_ref[...])
    v_ref[...] = v
    zero = [jnp.zeros((1, LANES), F32)] * 2
    yrows = joined(at_ref, arow_ref, frow_ref, ycount) + zero
    xrows = joined(at_ref, acol_ref, fcol_ref) + zero
    out_ref[count:, :] = jnp.concatenate(yrows + xrows, axis=0)
    places = jnp.concatenate(xrows + yrows, axis=0)
    select_rows(gf_ref, turned_places(odd, places, v.shape[0]))
    forward_left(v, gf_ref, l_ref)
    finish = forward_finish(out_ref)
    blocks = chunk // TILES

    def products(step):
        for inner in range(blocks):
            one_block(wt_ref, l_ref, step * blocks + inner, finish)

    def split(step):
        wait_chunk(step, chunk, copies, a_ref, held_ref, sems)
        for t in range(chunk):
            pair, at = (step * chunk + t) // 2, (t % 2) * LANES
            high, low = split2(held_ref[step * chunk + t].T)
            wt_ref[pair, at : at + LANES, :LANES] = high
            wt_ref[pair, at : at + LANES, LANES:] = low

    split(0)

    def body(step, carry):
        products(step - 1)
        split(step)
        return carry

    lax.fori_loop(1, len(copies), body, 0)
    products(len(copies) - 1)


def first_backward_kernel(n_col, ycount, acount, *refs):
    rho_ref, *refs = refs
    part_refs, refs = refs[:n_col], refs[n_col:]
    (w_ref, sq_ref, slack_ref, dual_ref), refs = refs[:4], refs[4:]
    mine_ref, theirs_ref, y_ref, s_ref, gb_ref, sb_ref, l_ref, rows_ref = refs
    rho, odd = rho_ref[0], odd_core()
    count = s_ref.shape[2]
    for j, ref in enumerate(part_refs):
        select_columns(s_ref.at[j], ref[count:, :])
    places = part_refs[0][count:, :]
    select_rows(gb_ref, places)
    select_columns(sb_ref, turned_places(odd, places[4:], sb_ref.shape[0]))
    full = gathered_rows(part_refs, s_ref)
    y_ref[...] = full
    top = rho * slack_ref[...] - dual_ref[...] - rho * full[:ycount]
    vec = jnp.concatenate([top, -full[ycount:]], axis=0)
    total = backward_sum(vec, gb_ref, sb_ref, w_ref, l_ref, rows_ref)
    squares = sq_ref[...]
    is_a = lax.broadcasted_iota(jnp.int32, squares.shape, 0) < acount
    parts = split3(jnp.where(is_a, rho * squares, squares))
    squares = sum(dot(sb_ref[...], part) for part in parts)
    half = total.shape[0] // 2
    mine_ref[:half, :] = total[:half]
    mine_ref[half:, :] = squares[:half]
    theirs_ref[:half, :] = total[half:]
    theirs_ref[half:, :] = squares[half:]


def finish_forward(u, p, resid, shifted, out_ref, gf_ref, w_ref, l_ref):
    count = 2 * w_ref.shape[0]
    weighted = shifted * u
    rows = [half_sum(resid * u), half_sum(weighted * u)]
    if p is not None:
        rows.append(half_sum(weighted * p))
    out_ref[count:, :] = pad_rows(rows)
    forward_parts(u, gf_ref, w_ref, out_ref, l_ref)


def second_forward_kernel(mine_ref, theirs_ref, v_ref, d_in_ref, c_in_ref, gf_ref, w_ref, *refs):
    r_ref, u_ref, pre_ref, d_ref, c_ref, out_ref, l_ref = refs
    odd = odd_core()
    half = v_ref.shape[0] // 2
    total = jnp.concatenate([mine_ref[:half, :], theirs_ref[:half, :]], axis=0)
    squares = jnp.concatenate([mine_ref[half:, :], theirs_ref[half:, :]], axis=0)
    v, d, c = v_ref[...], turn(odd, d_in_ref[...]), turn(odd, c_in_ref[...])
    d_ref[...] = d
    c_ref[...] = c
    resid = total - c - d * v
    shifted = d + SIGMA
    pre = shifted + squares
    u = resid / pre
    r_ref[...] = resid
    u_ref[...] = u
    pre_ref[...] = pre
    finish_forward(u, None, resid, shifted, out_ref, gf_ref, w_ref, l_ref)


def step_scalars(first, part_refs, sc_old_ref, count):
    totals = jnp.sum(tree(ref[count:, :] for ref in part_refs), axis=1, keepdims=True)
    gamma, one, two = totals[0:1], totals[1:2], totals[2:3]
    if first:
        return gamma, jnp.zeros_like(gamma), one
    old = sc_old_ref[...]
    beta = gamma / old[0:1, 0:1]
    return gamma, beta, one + beta * (2.0 * two + beta * old[2:3, 0:1])


def wide(x):
    return jnp.broadcast_to(x, (1, LANES))


def backward_kernel(n_col, ycount, first, last, *refs):
    rho_ref, *refs = refs
    part_refs, refs = refs[:n_col], refs[n_col:]
    s_ref, refs = refs[0], refs[1:]
    sc_old_ref = None
    if not first:
        (yp_old_ref, yv_old_ref, sc_old_ref, alpha_ref), refs = refs[:4], refs[4:]
    else:
        (yv_old_ref,), refs = refs[:1], refs[1:]
    if not last:
        (gb_ref, sb_ref, w_ref), refs = refs[:3], refs[3:]
    if last:
        z_ref, *refs = refs
    else:
        mine_ref, theirs_ref, *refs = refs
    yp_ref, yv_ref, sc_ref, *scratch = refs
    rho = rho_ref[0]
    full = gathered_rows(part_refs, s_ref)
    gamma, beta, pdp = step_scalars(first, part_refs, sc_old_ref, s_ref.shape[2])
    sc_ref[...] = pad_rows([wide(gamma), wide(beta), wide(pdp)])
    if first:
        yp = full
        yv_ref[...] = yv_old_ref[...]
    else:
        yp_old = yp_old_ref[...]
        yp = full + beta * yp_old
        yv_ref[...] = yv_old_ref[...] + alpha_ref[0:1, 0:1] * yp_old
    yp_ref[...] = yp
    scaled = jnp.concatenate([rho * yp[:ycount], yp[ycount:]], axis=0)
    norm = pad_rows([row_sum(scaled * yp)])
    if last:
        z_ref[...] = norm
    else:
        put_halves((mine_ref, theirs_ref), backward_sum(scaled, gb_ref, sb_ref, w_ref, *scratch), norm)


def step_alpha(extra, sc_ref):
    norm = jnp.sum(extra[0:1], axis=1, keepdims=True)
    return sc_ref[0:1, 0:1] / (sc_ref[2:3, 0:1] + norm)


def forward_kernel(first, *refs):
    (mine_ref, theirs_ref), refs = refs[:2], refs[2:]
    if not first:
        p_old_ref, refs = refs[0], refs[1:]
    (u_old_ref, v_old_ref, r_old_ref, d_ref, pre_ref, sc_ref, gf_ref, w_ref), refs = refs[:8], refs[8:]
    p_ref, v_ref, r_ref, u_ref, alpha_ref, out_ref, *scratch = refs
    half = d_ref.shape[0] // 2
    total = jnp.concatenate([mine_ref[:half, :], theirs_ref[:half, :]], axis=0)
    alpha = step_alpha(mine_ref[half:, :], sc_ref)
    p = u_old_ref[...]
    if not first:
        p = p + sc_ref[1:2, 0:1] * p_old_ref[...]
    shifted = d_ref[...] + SIGMA
    resid = r_old_ref[...] - alpha * (shifted * p + total)
    u = resid / pre_ref[...]
    p_ref[...] = p
    v_ref[...] = v_old_ref[...] + alpha * p
    r_ref[...] = resid
    u_ref[...] = u
    alpha_ref[...] = jnp.broadcast_to(alpha, (8, LANES))
    finish_forward(u, p, resid, shifted, out_ref, gf_ref, w_ref, *scratch)


def final_kernel(ycount, *refs):
    rho_ref, t_ref, *refs = refs
    (u_ref, p_old_ref, v_ref, start_ref, sc_ref, yp_ref, yv_ref, y0_ref), refs = refs[:8], refs[8:]
    (slack_ref, dual_ref, lower_ref, upper_ref, gb_ref, sb_ref, w_ref), refs = refs[:7], refs[7:]
    primal_out, half_out, slack_out, dual_out, mine_ref, theirs_ref, *scratch = refs
    rho = rho_ref[0]
    alpha = step_alpha(t_ref[...], sc_ref)
    p = u_ref[...] + sc_ref[1:2, 0:1] * p_old_ref[...]
    v = v_ref[...] + alpha * p
    primal = RELAX * v + (1.0 - RELAX) * start_ref[...]
    primal_out[...] = turn(odd_core(), primal)
    half_out[...] = primal[: primal.shape[0] // 2]
    image = yv_ref[...] + alpha * yp_ref[...]
    image_next = RELAX * image + (1.0 - RELAX) * y0_ref[...]
    dual = dual_ref[...]
    relaxed = RELAX * image[:ycount] + (1.0 - RELAX) * slack_ref[...]
    slack_next = jnp.minimum(jnp.maximum(relaxed + dual / rho, lower_ref[...]), upper_ref[...])
    dual_next = dual + rho * (relaxed - slack_next)
    slack_out[...] = slack_next
    dual_out[...] = dual_next
    worst = jnp.max(jnp.abs(image_next[:ycount] - slack_next), axis=0, keepdims=True)
    vec = jnp.concatenate([dual_next, image_next[ycount:]], axis=0)
    total = backward_sum(vec, gb_ref, sb_ref, w_ref, *scratch)
    put_halves((mine_ref, theirs_ref), total, jnp.broadcast_to(worst, (8, LANES)))


def residual_kernel(z_ref, primal_ref, d_ref, c_ref, out_ref):
    half = d_ref.shape[0] // 2
    dvec = d_ref[:half, :] * primal_ref[...] + z_ref[:half, :] + c_ref[:half, :]
    worst = jnp.max(jnp.abs(dvec), axis=0, keepdims=True)
    out_ref[...] = jnp.concatenate([z_ref[half : half + 4, :], jnp.broadcast_to(worst, (4, LANES))], axis=0)


VMEM_SPEC = pl.BlockSpec(memory_space=pltpu.VMEM)
SMEM_SPEC = pl.BlockSpec(memory_space=pltpu.SMEM)
HBM_SPEC = pl.BlockSpec(memory_space=pltpu.HBM)


def call(kernel, name, outs, args, scratch=(), scalars=0, streamed=0, cost=None):
    kinds = [SMEM_SPEC] * scalars + [HBM_SPEC] * streamed
    specs = kinds + [VMEM_SPEC] * (len(args) - len(kinds))
    args = [
        pltpu.with_memory_space_constraint(x, pltpu.HBM) if scalars <= i < scalars + streamed else x
        for i, x in enumerate(args)
    ]
    shapes = tuple(s if isinstance(s, jax.ShapeDtypeStruct) else jax.ShapeDtypeStruct(s, F32) for s in outs)
    return pl.pallas_call(
        kernel,
        out_shape=shapes,
        in_specs=specs,
        out_specs=tuple(VMEM_SPEC for _ in outs),
        scratch_shapes=list(scratch),
        compiler_params=pltpu.CompilerParams(vmem_limit_bytes=VMEM_LIMIT),
        cost_estimate=cost,
        name=name,
    )(*args)


def swap(x, axis, size, distance):
    return lax.ppermute(x, axis, [(i, i ^ distance) for i in range(size)])


def exchange(x, axis, size, distances):
    return [x] + [swap(x, axis, size, m) for m in distances]


def local(n_row, n_col, *args):
    (
        constraint_tiles,
        constraint_rows,
        constraint_cols,
        factor_tiles,
        factor_rows,
        factor_cols,
        diag_cost,
        linear_cost,
        lower_bound,
        upper_bound,
        primal_start,
        slack_start,
        dual_start,
        penalty,
    ) = args
    width = constraint_tiles.shape[2]
    ctiles = constraint_tiles.reshape(-1, width, width)
    ftiles = factor_tiles.reshape(-1, width, width)
    acount, fcount = ctiles.shape[0], ftiles.shape[0]
    count = acount + fcount
    pairs = count // 2
    xcount = primal_start.shape[0]
    ycount = slack_start.shape[0]
    full = ycount + YG
    half = xcount // 2

    def over_col(x):
        return exchange(x, "col", n_col, sorted(range(1, n_col), key=lambda m: (m != 2, m)))

    def over_plane(chip, op=jnp.add):
        return tree(exchange(chip, "row", n_row, range(2, n_row, 2)), op)

    def other_core(x):
        return swap(x, "row", n_row, 1)

    def over_row(mine, theirs):
        summed = over_plane(mine + other_core(theirs))
        return summed, other_core(summed)

    rho = penalty.reshape(1)
    chunk = next(n for n in (24, 16, 8) if acount % n == 0 and fcount % n == 0)
    assert acount <= width and fcount <= width
    matrices = jax.ShapeDtypeStruct((pairs, 2 * width, 2 * width), BF16)
    held = [
        pltpu.VMEM((count, width, width), F32),
        pltpu.SemaphoreType.DMA((count // chunk,)),
    ]

    left = pltpu.VMEM((2 * count, 2 * width), BF16)
    rows = pltpu.VMEM((count, width), F32)
    xs, ys, small = (xcount, width), (full, width), (8, width)
    sent, summed = (count + 8, width), (half + 8, width)
    bits = functools.partial(jax.ShapeDtypeStruct, dtype=BF16)

    turned, parts, start, gf = call(
        functools.partial(first_forward_kernel, chunk, ycount),
        "first_forward",
        [matrices, sent, xs, bits((count, xcount))],
        (rho, ctiles, ftiles, primal_start)
        + tuple(x.reshape(1, -1) for x in (constraint_rows, constraint_cols, factor_rows, factor_cols)),
        [left, pltpu.VMEM((8, width), F32), pltpu.VMEM(xs, F32)]
        + [pltpu.VMEM((1, n), jnp.int32) for n in (acount, acount, fcount, fcount)]
        + [pltpu.SemaphoreType.DMA((5,)), *held],
        scalars=1,
        streamed=7,
    )
    parts, ctiles, ftiles = lax.optimization_barrier((parts, ctiles, ftiles))
    all_parts = over_col(parts)
    tiles, squares = call(
        functools.partial(split_kernel, chunk),
        "split",
        [matrices, (count, width)],
        (ctiles, ftiles),
        held,
        streamed=2,
        cost=pl.CostEstimate(
            flops=8 * count * width * width, bytes_accessed=4 * count * width * width, transcendentals=0
        ),
    )
    mine, theirs, y0, s_all, gb, sb = call(
        functools.partial(first_backward_kernel, n_col, ycount, acount),
        "first_backward",
        [xs, xs, ys, bits((n_col, full, count)), bits((count, full)), bits((xcount, count))],
        (rho, *all_parts, tiles, squares, slack_start, dual_start),
        [left, rows],
        scalars=1,
    )
    resid, u, precond, diag, linear, parts = call(
        second_forward_kernel,
        "second_forward",
        [xs, xs, xs, xs, xs, sent],
        (*over_row(mine, theirs), start, diag_cost, linear_cost, gf, turned),
        [left],
    )
    v, yv = start, y0
    p = yp = sc = alpha = None
    for step in range(CG):
        first, last = step == 0, step + 1 == CG
        state = (yv,) if first else (yp, yv, sc, alpha)
        mats = () if last else (gb, sb, tiles)
        *z, yp, yv, sc = call(
            functools.partial(backward_kernel, n_col, ycount, first, last),
            "last_norm" if last else "backward",
            ([small] if last else [summed, summed]) + [ys, ys, small],
            (rho, *over_col(parts), s_all, *state, *mats),
            [] if last else [left, rows],
            scalars=1,
        )
        if last:
            break
        p, v, resid, u, alpha, parts = call(
            functools.partial(forward_kernel, first),
            "forward",
            [xs, xs, xs, xs, small, sent],
            (*over_row(*z), *(() if first else (p,)), u, v, resid, diag, precond, sc, gf, turned),
            [left],
        )
    norm = over_plane(z[0] + other_core(z[0]))
    primal_next, primal_half, slack_next, dual_next, mine, theirs = call(
        functools.partial(final_kernel, ycount),
        "final",
        [xs, (half, width), (ycount, width), (ycount, width), summed, summed],
        (rho, norm, u, p, v, start, sc, yp, yv, y0)
        + (slack_start, dual_start, lower_bound, upper_bound, gb, sb, tiles),
        [left, rows],
        scalars=1,
    )

    def join(a, b):
        is_sum = lax.broadcasted_iota(jnp.int32, a.shape, 0) < half
        return jnp.where(is_sum, a + b, jnp.maximum(a, b))

    z = over_plane(join(mine, other_core(theirs)), join)
    (worst,) = call(residual_kernel, "residuals", [small], (z, primal_half, diag, linear))
    worst = jnp.maximum(worst, other_core(worst))
    worst = tree(exchange(worst, "col", n_col, range(1, n_col)), jnp.maximum)
    return (primal_next, slack_next, dual_next, jnp.max(worst[:4]), jnp.max(worst[4:]))


def solution(mesh):
    placed = (
        P("row", "col", None, None),
        P("row", "col"),
        P("row", "col"),
        P("row", "col", None, None),
        P("row", "col"),
        P("row", "col"),
        P("col", None),
        P("col", None),
        P("row", None),
        P("row", None),
        P("col", None),
        P("row", None),
        P("row", None),
        P(),
    )
    return jax.shard_map(
        functools.partial(local, mesh.shape["row"], mesh.shape["col"]),
        mesh=mesh,
        in_specs=placed,
        out_specs=(P("col", None), P("row", None), P("row", None), P(), P()),
        check_vma=False,
    )
```

```python
import functools

import jax
import jax.numpy as jnp
from jax import lax
from jax.experimental import pallas as pl
from jax.experimental.pallas import tpu as pltpu
from jax.sharding import PartitionSpec as P

YG = 64
CG = 6

SIGMA = 1e-06
RELAX = 1.6

F32 = jnp.float32
BF16 = jnp.bfloat16
LANES = 128
UNROLL = 18
IN_FLIGHT = 4
LANES = 128
TILES = 8
VMEM_LIMIT = 24 * 1024 * 1024


def dot(a, b):
    return lax.dot_general(a, b, (((1,), (0,)), ((), ())), preferred_element_type=F32)


def split2(x):
    high = x.astype(BF16)
    return high, (x - high.astype(F32)).astype(BF16)


def split3(x):
    high = x.astype(BF16)
    return (high, *split2(x - high.astype(F32)))


def tree(parts, op=jnp.add):
    parts = list(parts)
    while len(parts) > 1:
        parts = [op(parts[i], parts[i + 1]) for i in range(0, len(parts), 2)]
    return parts[0]


def row_sum(x):
    return jnp.sum(x, axis=0, keepdims=True)


def half_sum(x):
    half = x.shape[0] // 2
    return row_sum(x[:half]) + row_sum(x[half:])


def turn(odd, x):
    half = x.shape[0] // 2
    return jnp.where(odd, jnp.concatenate([x[half:], x[:half]], axis=0), x)


def pad_rows(rows):
    return jnp.concatenate(list(rows) + [jnp.zeros((8 - len(rows), LANES), F32)], axis=0)


def gather(onehot_ref, x):
    both = dot(onehot_ref[...], jnp.concatenate(split2(x), axis=1))
    high, low = both[:, :LANES], both[:, LANES:]
    blocks = high.shape[0] // TILES
    shape = (blocks, TILES, LANES)
    return jnp.concatenate([high.reshape(shape), low.reshape(shape)], axis=1).reshape(2 * TILES * blocks, LANES)


def scatter(onehot, x):
    both = dot(onehot, jnp.concatenate(split2(x), axis=1))
    return both[:, :LANES] + both[:, LANES:]


def one_block(w_ref, l_ref, block, finish):
    pairs = TILES // 2
    of_pair = lax.broadcasted_iota(jnp.int32, (2 * TILES, 2 * LANES), 0) % TILES // 2
    left = l_ref[pl.ds(pl.multiple_of(block * 2 * TILES, 2 * TILES), 2 * TILES), :]
    out = dot(left, w_ref[pairs * block])
    for k in range(1, pairs):
        out = jnp.where(of_pair == k, dot(left, w_ref[pairs * block + k]), out)
    finish(pl.multiple_of(block * TILES, TILES), out[:TILES] + out[TILES:])


def run_tiles(w_ref, l_ref, most, finish):
    blocks = w_ref.shape[0] // (TILES // 2)
    unroll = next(n for n in (most, 6, 4, 3, 2, 1) if blocks % n == 0)

    def body(step, carry):
        for inner in range(unroll):
            one_block(w_ref, l_ref, step * unroll + inner, finish)
        return carry

    lax.fori_loop(0, blocks // unroll, body, 0)


def forward_left(vec, gf_ref, l_ref):
    picked = gather(gf_ref, vec)
    first = lax.broadcasted_iota(jnp.int32, picked.shape, 0) % 2 == 0
    zero = jnp.zeros_like(picked)
    l_ref[:, :LANES] = jnp.where(first, picked, zero).astype(BF16)
    l_ref[:, LANES:] = jnp.where(first, zero, picked).astype(BF16)


def forward_finish(out_ref):
    def finish(at, out):
        out_ref[pl.ds(at, TILES), :] = out[:, :LANES] + out[:, LANES:]

    return finish


def forward_parts(vec, gf_ref, wt_ref, out_ref, l_ref):
    forward_left(vec, gf_ref, l_ref)
    run_tiles(wt_ref, l_ref, UNROLL, forward_finish(out_ref))


def backward_sum(vec, gb_ref, sb_ref, w_ref, l_ref, rows_ref):
    picked = gather(gb_ref, vec).astype(BF16)
    l_ref[:, :LANES] = picked
    l_ref[:, LANES:] = picked
    first = lax.broadcasted_iota(jnp.int32, (TILES, LANES), 0) % 2 == 0

    def finish(at, out):
        rows_ref[pl.ds(at, TILES), :] = jnp.where(first, out[:, :LANES], out[:, LANES:])

    run_tiles(w_ref, l_ref, UNROLL, finish)
    return scatter(sb_ref[...], rows_ref[...])


def gathered_rows(part_refs, s_ref):
    count = s_ref.shape[2]
    return tree(scatter(s_ref[j], ref[:count, :]) for j, ref in enumerate(part_refs))


def put_halves(refs, total, extra):
    half = total.shape[0] // 2
    for ref, part in zip(refs, (total[:half], total[half:])):
        ref[:half, :] = part
        ref[half:, :] = extra


def select_columns(ref, rows):
    size, count = ref.shape
    for row in range(pl.cdiv(count, LANES)):
        width = min(LANES, count - row * LANES)
        hit = lax.broadcasted_iota(jnp.int32, (size, width), 0) == rows[row : row + 1, :width].astype(jnp.int32)
        ref[:, row * LANES : row * LANES + width] = jnp.where(hit, 1.0, 0.0).astype(BF16)


def select_rows(ref, rows):
    count, size = ref.shape
    across = rows.T.astype(jnp.int32)
    for row in range(pl.cdiv(count, LANES)):
        width = min(LANES, count - row * LANES)
        hit = lax.broadcasted_iota(jnp.int32, (width, size), 1) == across[:width, row : row + 1]
        ref[row * LANES : row * LANES + width, :] = jnp.where(hit, 1.0, 0.0).astype(BF16)


def tile_copies(chunk, refs, held_ref, sems):
    copies, at = [], 0
    for ref in refs:
        for start in range(0, ref.shape[0], chunk):
            copies.append(
                pltpu.make_async_copy(
                    ref.at[pl.ds(start, chunk)], held_ref.at[pl.ds(at, chunk)], sems.at[len(copies)]
                )
            )
            at += chunk
    return copies


def wait_chunk(step, chunk, copies, a_ref, held_ref, sems):
    for later in range(IN_FLIGHT, len(copies)):
        pl.when(step + IN_FLIGHT == later)(copies[later].start)
    at = pl.multiple_of(step * chunk, chunk)
    pltpu.make_async_copy(a_ref.at[pl.ds(0, chunk)], held_ref.at[pl.ds(at, chunk)], sems.at[step]).wait()


def odd_core():
    return lax.axis_index("row") % 2 == 1


def split_kernel(chunk, a_ref, g_ref, w_ref, sq_ref, held_ref, sems):
    copies = tile_copies(chunk, (a_ref, g_ref), held_ref, sems)
    for copy in copies:
        copy.start()

    def body(step, carry):
        wait_chunk(step, chunk, (), a_ref, held_ref, sems)
        for t in range(chunk):
            tile = held_ref[step * chunk + t]
            pair, at = (step * chunk + t) // 2, (t % 2) * LANES
            high, low = split2(tile)
            w_ref[pair, :LANES, at : at + LANES] = high
            w_ref[pair, LANES:, at : at + LANES] = low
            sq_ref[pl.ds(step * chunk + t, 1), :] = row_sum(tile * tile)
        return carry

    lax.fori_loop(0, len(copies), body, 0)


def turned_places(odd, places, xcount):
    half = xcount // 2
    moved = jnp.where(places >= half, places - half, places + half)
    return jnp.where(odd, moved, places)


def joined(at_ref, a_ref, f_ref, base=0):
    acount, fcount = a_ref.shape[1], f_ref.shape[1]
    at_ref[...] = jnp.zeros_like(at_ref)
    at_ref[0:1, :acount] = a_ref[...].astype(F32)
    at_ref[1:2, :fcount] = (f_ref[...] + base).astype(F32)
    a, f = at_ref[0:1, :], at_ref[1:2, :]
    moved = pltpu.roll(jnp.broadcast_to(f, (8, LANES)), acount % LANES, 1)[0:1]
    lane = lax.broadcasted_iota(jnp.int32, (1, LANES), 1)
    return [jnp.where(lane < acount, a, moved), moved]


def first_forward_kernel(chunk, ycount, rho_ref, *refs):
    (a_ref, g_ref), small_refs, refs = refs[:2], refs[2:7], refs[7:]
    (wt_ref, out_ref, v_ref, gf_ref, l_ref, at_ref), refs = refs[:6], refs[6:]
    small_held, (small_sems, held_ref, sems) = refs[:5], refs[5:]
    fetched = [pltpu.make_async_copy(a, b, small_sems.at[i]) for i, (a, b) in enumerate(zip(small_refs, small_held))]
    copies = tile_copies(chunk, (a_ref, g_ref), held_ref, sems)
    for copy in fetched + copies[:1]:
        copy.start()
    odd = odd_core()
    for copy in fetched:
        copy.wait()
    for copy in copies[1:IN_FLIGHT]:
        copy.start()
    v_in_ref, arow_ref, acol_ref, frow_ref, fcol_ref = small_held
    count = 2 * wt_ref.shape[0]
    v = turn(odd, v_in_ref[...])
    v_ref[...] = v
    zero = [jnp.zeros((1, LANES), F32)] * 2
    yrows = joined(at_ref, arow_ref, frow_ref, ycount) + zero
    xrows = joined(at_ref, acol_ref, fcol_ref) + zero
    out_ref[count:, :] = jnp.concatenate(yrows + xrows, axis=0)
    places = jnp.concatenate(xrows + yrows, axis=0)
    select_rows(gf_ref, turned_places(odd, places, v.shape[0]))
    forward_left(v, gf_ref, l_ref)
    finish = forward_finish(out_ref)

    def split(step):
        wait_chunk(step, chunk, copies, a_ref, held_ref, sems)
        for t in range(chunk):
            pair, at = (step * chunk + t) // 2, (t % 2) * LANES
            high, low = split2(held_ref[step * chunk + t].T)
            wt_ref[pair, at : at + LANES, :LANES] = high
            wt_ref[pair, at : at + LANES, LANES:] = low

    def body(step, carry):
        split(step)
        return carry

    lax.fori_loop(0, len(copies), body, 0)
    run_tiles(wt_ref, l_ref, UNROLL, finish)


def first_backward_kernel(n_col, ycount, acount, *refs):
    rho_ref, *refs = refs
    part_refs, refs = refs[:n_col], refs[n_col:]
    (w_ref, sq_ref, slack_ref, dual_ref), refs = refs[:4], refs[4:]
    mine_ref, theirs_ref, y_ref, s_ref, gb_ref, sb_ref, l_ref, rows_ref = refs
    rho, odd = rho_ref[0], odd_core()
    count = s_ref.shape[2]
    for j, ref in enumerate(part_refs):
        select_columns(s_ref.at[j], ref[count:, :])
    places = part_refs[0][count:, :]
    select_rows(gb_ref, places)
    select_columns(sb_ref, turned_places(odd, places[4:], sb_ref.shape[0]))
    full = gathered_rows(part_refs, s_ref)
    y_ref[...] = full
    top = rho * slack_ref[...] - dual_ref[...] - rho * full[:ycount]
    vec = jnp.concatenate([top, -full[ycount:]], axis=0)
    total = backward_sum(vec, gb_ref, sb_ref, w_ref, l_ref, rows_ref)
    squares = sq_ref[...]
    is_a = lax.broadcasted_iota(jnp.int32, squares.shape, 0) < acount
    parts = split3(jnp.where(is_a, rho * squares, squares))
    squares = sum(dot(sb_ref[...], part) for part in parts)
    half = total.shape[0] // 2
    mine_ref[:half, :] = total[:half]
    mine_ref[half:, :] = squares[:half]
    theirs_ref[:half, :] = total[half:]
    theirs_ref[half:, :] = squares[half:]


def finish_forward(u, p, resid, shifted, out_ref, gf_ref, w_ref, l_ref):
    count = 2 * w_ref.shape[0]
    weighted = shifted * u
    rows = [half_sum(resid * u), half_sum(weighted * u)]
    if p is not None:
        rows.append(half_sum(weighted * p))
    out_ref[count:, :] = pad_rows(rows)
    forward_parts(u, gf_ref, w_ref, out_ref, l_ref)


def second_forward_kernel(mine_ref, theirs_ref, v_ref, d_in_ref, c_in_ref, gf_ref, w_ref, *refs):
    r_ref, u_ref, pre_ref, d_ref, c_ref, out_ref, l_ref = refs
    odd = odd_core()
    half = v_ref.shape[0] // 2
    total = jnp.concatenate([mine_ref[:half, :], theirs_ref[:half, :]], axis=0)
    squares = jnp.concatenate([mine_ref[half:, :], theirs_ref[half:, :]], axis=0)
    v, d, c = v_ref[...], turn(odd, d_in_ref[...]), turn(odd, c_in_ref[...])
    d_ref[...] = d
    c_ref[...] = c
    resid = total - c - d * v
    shifted = d + SIGMA
    pre = shifted + squares
    u = resid / pre
    r_ref[...] = resid
    u_ref[...] = u
    pre_ref[...] = pre
    finish_forward(u, None, resid, shifted, out_ref, gf_ref, w_ref, l_ref)


def step_scalars(first, part_refs, sc_old_ref, count):
    totals = jnp.sum(tree(ref[count:, :] for ref in part_refs), axis=1, keepdims=True)
    gamma, one, two = totals[0:1], totals[1:2], totals[2:3]
    if first:
        return gamma, jnp.zeros_like(gamma), one
    old = sc_old_ref[...]
    beta = gamma / old[0:1, 0:1]
    return gamma, beta, one + beta * (2.0 * two + beta * old[2:3, 0:1])


def wide(x):
    return jnp.broadcast_to(x, (1, LANES))


def backward_kernel(n_col, ycount, first, last, *refs):
    rho_ref, *refs = refs
    part_refs, refs = refs[:n_col], refs[n_col:]
    s_ref, refs = refs[0], refs[1:]
    sc_old_ref = None
    if not first:
        (yp_old_ref, yv_old_ref, sc_old_ref, alpha_ref), refs = refs[:4], refs[4:]
    else:
        (yv_old_ref,), refs = refs[:1], refs[1:]
    if not last:
        (gb_ref, sb_ref, w_ref), refs = refs[:3], refs[3:]
    if last:
        z_ref, *refs = refs
    else:
        mine_ref, theirs_ref, *refs = refs
    yp_ref, yv_ref, sc_ref, *scratch = refs
    rho = rho_ref[0]
    full = gathered_rows(part_refs, s_ref)
    gamma, beta, pdp = step_scalars(first, part_refs, sc_old_ref, s_ref.shape[2])
    sc_ref[...] = pad_rows([wide(gamma), wide(beta), wide(pdp)])
    if first:
        yp = full
        yv_ref[...] = yv_old_ref[...]
    else:
        yp_old = yp_old_ref[...]
        yp = full + beta * yp_old
        yv_ref[...] = yv_old_ref[...] + alpha_ref[0:1, 0:1] * yp_old
    yp_ref[...] = yp
    scaled = jnp.concatenate([rho * yp[:ycount], yp[ycount:]], axis=0)
    norm = pad_rows([row_sum(scaled * yp)])
    if last:
        z_ref[...] = norm
    else:
        put_halves((mine_ref, theirs_ref), backward_sum(scaled, gb_ref, sb_ref, w_ref, *scratch), norm)


def step_alpha(extra, sc_ref):
    norm = jnp.sum(extra[0:1], axis=1, keepdims=True)
    return sc_ref[0:1, 0:1] / (sc_ref[2:3, 0:1] + norm)


def forward_kernel(first, *refs):
    (mine_ref, theirs_ref), refs = refs[:2], refs[2:]
    if not first:
        p_old_ref, refs = refs[0], refs[1:]
    (u_old_ref, v_old_ref, r_old_ref, d_ref, pre_ref, sc_ref, gf_ref, w_ref), refs = refs[:8], refs[8:]
    p_ref, v_ref, r_ref, u_ref, alpha_ref, out_ref, *scratch = refs
    half = d_ref.shape[0] // 2
    total = jnp.concatenate([mine_ref[:half, :], theirs_ref[:half, :]], axis=0)
    alpha = step_alpha(mine_ref[half:, :], sc_ref)
    p = u_old_ref[...]
    if not first:
        p = p + sc_ref[1:2, 0:1] * p_old_ref[...]
    shifted = d_ref[...] + SIGMA
    resid = r_old_ref[...] - alpha * (shifted * p + total)
    u = resid / pre_ref[...]
    p_ref[...] = p
    v_ref[...] = v_old_ref[...] + alpha * p
    r_ref[...] = resid
    u_ref[...] = u
    alpha_ref[...] = jnp.broadcast_to(alpha, (8, LANES))
    finish_forward(u, p, resid, shifted, out_ref, gf_ref, w_ref, *scratch)


def final_kernel(ycount, *refs):
    rho_ref, t_ref, *refs = refs
    (u_ref, p_old_ref, v_ref, start_ref, sc_ref, yp_ref, yv_ref, y0_ref), refs = refs[:8], refs[8:]
    (slack_ref, dual_ref, lower_ref, upper_ref, gb_ref, sb_ref, w_ref), refs = refs[:7], refs[7:]
    primal_out, half_out, slack_out, dual_out, mine_ref, theirs_ref, *scratch = refs
    rho = rho_ref[0]
    alpha = step_alpha(t_ref[...], sc_ref)
    p = u_ref[...] + sc_ref[1:2, 0:1] * p_old_ref[...]
    v = v_ref[...] + alpha * p
    primal = RELAX * v + (1.0 - RELAX) * start_ref[...]
    primal_out[...] = turn(odd_core(), primal)
    half_out[...] = primal[: primal.shape[0] // 2]
    image = yv_ref[...] + alpha * yp_ref[...]
    image_next = RELAX * image + (1.0 - RELAX) * y0_ref[...]
    dual = dual_ref[...]
    relaxed = RELAX * image[:ycount] + (1.0 - RELAX) * slack_ref[...]
    slack_next = jnp.minimum(jnp.maximum(relaxed + dual / rho, lower_ref[...]), upper_ref[...])
    dual_next = dual + rho * (relaxed - slack_next)
    slack_out[...] = slack_next
    dual_out[...] = dual_next
    worst = jnp.max(jnp.abs(image_next[:ycount] - slack_next), axis=0, keepdims=True)
    vec = jnp.concatenate([dual_next, image_next[ycount:]], axis=0)
    total = backward_sum(vec, gb_ref, sb_ref, w_ref, *scratch)
    put_halves((mine_ref, theirs_ref), total, jnp.broadcast_to(worst, (8, LANES)))


def residual_kernel(z_ref, primal_ref, d_ref, c_ref, out_ref):
    half = d_ref.shape[0] // 2
    dvec = d_ref[:half, :] * primal_ref[...] + z_ref[:half, :] + c_ref[:half, :]
    worst = jnp.max(jnp.abs(dvec), axis=0, keepdims=True)
    out_ref[...] = jnp.concatenate([z_ref[half : half + 4, :], jnp.broadcast_to(worst, (4, LANES))], axis=0)


VMEM_SPEC = pl.BlockSpec(memory_space=pltpu.VMEM)
SMEM_SPEC = pl.BlockSpec(memory_space=pltpu.SMEM)
HBM_SPEC = pl.BlockSpec(memory_space=pltpu.HBM)


def call(kernel, name, outs, args, scratch=(), scalars=0, streamed=0, cost=None):
    kinds = [SMEM_SPEC] * scalars + [HBM_SPEC] * streamed
    specs = kinds + [VMEM_SPEC] * (len(args) - len(kinds))
    args = [
        pltpu.with_memory_space_constraint(x, pltpu.HBM) if scalars <= i < scalars + streamed else x
        for i, x in enumerate(args)
    ]
    shapes = tuple(s if isinstance(s, jax.ShapeDtypeStruct) else jax.ShapeDtypeStruct(s, F32) for s in outs)
    return pl.pallas_call(
        kernel,
        out_shape=shapes,
        in_specs=specs,
        out_specs=tuple(VMEM_SPEC for _ in outs),
        scratch_shapes=list(scratch),
        compiler_params=pltpu.CompilerParams(vmem_limit_bytes=VMEM_LIMIT),
        cost_estimate=cost,
        name=name,
    )(*args)


def swap(x, axis, size, distance):
    return lax.ppermute(x, axis, [(i, i ^ distance) for i in range(size)])


def exchange(x, axis, size, distances):
    return [x] + [swap(x, axis, size, m) for m in distances]


def local(n_row, n_col, *args):
    (
        constraint_tiles,
        constraint_rows,
        constraint_cols,
        factor_tiles,
        factor_rows,
        factor_cols,
        diag_cost,
        linear_cost,
        lower_bound,
        upper_bound,
        primal_start,
        slack_start,
        dual_start,
        penalty,
    ) = args
    width = constraint_tiles.shape[2]
    ctiles = constraint_tiles.reshape(-1, width, width)
    ftiles = factor_tiles.reshape(-1, width, width)
    acount, fcount = ctiles.shape[0], ftiles.shape[0]
    count = acount + fcount
    pairs = count // 2
    xcount = primal_start.shape[0]
    ycount = slack_start.shape[0]
    full = ycount + YG
    half = xcount // 2

    def over_col(x):
        return exchange(x, "col", n_col, sorted(range(1, n_col), key=lambda m: (m != 2, m)))

    def over_plane(chip, op=jnp.add):
        return tree(exchange(chip, "row", n_row, range(2, n_row, 2)), op)

    def other_core(x):
        return swap(x, "row", n_row, 1)

    def over_row(mine, theirs):
        summed = over_plane(mine + other_core(theirs))
        return summed, other_core(summed)

    rho = penalty.reshape(1)
    chunk = next(n for n in (24, 16, 8) if acount % n == 0 and fcount % n == 0)
    assert acount <= width and fcount <= width
    matrices = jax.ShapeDtypeStruct((pairs, 2 * width, 2 * width), BF16)
    held = [
        pltpu.VMEM((count, width, width), F32),
        pltpu.SemaphoreType.DMA((count // chunk,)),
    ]

    left = pltpu.VMEM((2 * count, 2 * width), BF16)
    rows = pltpu.VMEM((count, width), F32)
    xs, ys, small = (xcount, width), (full, width), (8, width)
    sent, summed = (count + 8, width), (half + 8, width)
    bits = functools.partial(jax.ShapeDtypeStruct, dtype=BF16)

    turned, parts, start, gf = call(
        functools.partial(first_forward_kernel, chunk, ycount),
        "first_forward",
        [matrices, sent, xs, bits((count, xcount))],
        (rho, ctiles, ftiles, primal_start)
        + tuple(x.reshape(1, -1) for x in (constraint_rows, constraint_cols, factor_rows, factor_cols)),
        [left, pltpu.VMEM((8, width), F32), pltpu.VMEM(xs, F32)]
        + [pltpu.VMEM((1, n), jnp.int32) for n in (acount, acount, fcount, fcount)]
        + [pltpu.SemaphoreType.DMA((5,)), *held],
        scalars=1,
        streamed=7,
    )
    parts, ctiles, ftiles = lax.optimization_barrier((parts, ctiles, ftiles))
    all_parts = over_col(parts)
    tiles, squares = call(
        functools.partial(split_kernel, chunk),
        "split",
        [matrices, (count, width)],
        (ctiles, ftiles),
        held,
        streamed=2,
        cost=pl.CostEstimate(
            flops=8 * count * width * width, bytes_accessed=4 * count * width * width, transcendentals=0
        ),
    )
    mine, theirs, y0, s_all, gb, sb = call(
        functools.partial(first_backward_kernel, n_col, ycount, acount),
        "first_backward",
        [xs, xs, ys, bits((n_col, full, count)), bits((count, full)), bits((xcount, count))],
        (rho, *all_parts, tiles, squares, slack_start, dual_start),
        [left, rows],
        scalars=1,
    )
    resid, u, precond, diag, linear, parts = call(
        second_forward_kernel,
        "second_forward",
        [xs, xs, xs, xs, xs, sent],
        (*over_row(mine, theirs), start, diag_cost, linear_cost, gf, turned),
        [left],
    )
    v, yv = start, y0
    p = yp = sc = alpha = None
    for step in range(CG):
        first, last = step == 0, step + 1 == CG
        state = (yv,) if first else (yp, yv, sc, alpha)
        mats = () if last else (gb, sb, tiles)
        *z, yp, yv, sc = call(
            functools.partial(backward_kernel, n_col, ycount, first, last),
            "last_norm" if last else "backward",
            ([small] if last else [summed, summed]) + [ys, ys, small],
            (rho, *over_col(parts), s_all, *state, *mats),
            [] if last else [left, rows],
            scalars=1,
        )
        if last:
            break
        p, v, resid, u, alpha, parts = call(
            functools.partial(forward_kernel, first),
            "forward",
            [xs, xs, xs, xs, small, sent],
            (*over_row(*z), *(() if first else (p,)), u, v, resid, diag, precond, sc, gf, turned),
            [left],
        )
    norm = over_plane(z[0] + other_core(z[0]))
    primal_next, primal_half, slack_next, dual_next, mine, theirs = call(
        functools.partial(final_kernel, ycount),
        "final",
        [xs, (half, width), (ycount, width), (ycount, width), summed, summed],
        (rho, norm, u, p, v, start, sc, yp, yv, y0)
        + (slack_start, dual_start, lower_bound, upper_bound, gb, sb, tiles),
        [left, rows],
        scalars=1,
    )

    def join(a, b):
        is_sum = lax.broadcasted_iota(jnp.int32, a.shape, 0) < half
        return jnp.where(is_sum, a + b, jnp.maximum(a, b))

    z = over_plane(join(mine, other_core(theirs)), join)
    (worst,) = call(residual_kernel, "residuals", [small], (z, primal_half, diag, linear))
    worst = jnp.maximum(worst, other_core(worst))
    if n_col == 4:
        def ask(even, odd):
            at = [(r, c) for r in range(n_row) for c in range(n_col)]
            pairs = [(r * n_col + c, r * n_col + (c ^ (odd if r % 2 else even))) for r, c in at]
            return lax.ppermute(worst, ("row", "col"), pairs)

        worst = tree((worst, ask(1, 2), ask(3, 3), worst), jnp.maximum)
        worst = jnp.maximum(worst, other_core(worst))
    else:
        worst = tree(exchange(worst, "col", n_col, range(1, n_col)), jnp.maximum)
    return (primal_next, slack_next, dual_next, jnp.max(worst[:4]), jnp.max(worst[4:]))


def solution(mesh):
    placed = (
        P("row", "col", None, None),
        P("row", "col"),
        P("row", "col"),
        P("row", "col", None, None),
        P("row", "col"),
        P("row", "col"),
        P("col", None),
        P("col", None),
        P("row", None),
        P("row", None),
        P("col", None),
        P("row", None),
        P("row", None),
        P(),
    )
    return jax.shard_map(
        functools.partial(local, mesh.shape["row"], mesh.shape["col"]),
        mesh=mesh,
        in_specs=placed,
        out_specs=(P("col", None), P("row", None), P("row", None), P(), P()),
        check_vma=False,
    )
```

```python
import functools

import jax
import jax.numpy as jnp
from jax import lax
from jax.experimental import pallas as pl
from jax.experimental.pallas import tpu as pltpu
from jax.sharding import PartitionSpec as P

YG = 64
CG = 6

SIGMA = 1e-06
RELAX = 1.6

F32 = jnp.float32
BF16 = jnp.bfloat16
LANES = 128
UNROLL = 18
IN_FLIGHT = 4
LANES = 128
TILES = 8
VMEM_LIMIT = 24 * 1024 * 1024


def dot(a, b):
    return lax.dot_general(a, b, (((1,), (0,)), ((), ())), preferred_element_type=F32)


def split2(x):
    high = x.astype(BF16)
    return high, (x - high.astype(F32)).astype(BF16)


def split3(x):
    high = x.astype(BF16)
    return (high, *split2(x - high.astype(F32)))


def tree(parts, op=jnp.add):
    parts = list(parts)
    while len(parts) > 1:
        parts = [op(parts[i], parts[i + 1]) for i in range(0, len(parts), 2)]
    return parts[0]


def row_sum(x):
    return jnp.sum(x, axis=0, keepdims=True)


def half_sum(x):
    half = x.shape[0] // 2
    return row_sum(x[:half]) + row_sum(x[half:])


def turn(odd, x):
    half = x.shape[0] // 2
    return jnp.where(odd, jnp.concatenate([x[half:], x[:half]], axis=0), x)


def pad_rows(rows):
    return jnp.concatenate(list(rows) + [jnp.zeros((8 - len(rows), LANES), F32)], axis=0)


def gather(onehot_ref, x):
    both = dot(onehot_ref[...], jnp.concatenate(split2(x), axis=1))
    high, low = both[:, :LANES], both[:, LANES:]
    blocks = high.shape[0] // TILES
    shape = (blocks, TILES, LANES)
    return jnp.concatenate([high.reshape(shape), low.reshape(shape)], axis=1).reshape(2 * TILES * blocks, LANES)


def scatter(onehot, x):
    both = dot(onehot, jnp.concatenate(split2(x), axis=1))
    return both[:, :LANES] + both[:, LANES:]


def one_block(w_ref, l_ref, block, finish):
    pairs = TILES // 2
    of_pair = lax.broadcasted_iota(jnp.int32, (2 * TILES, 2 * LANES), 0) % TILES // 2
    left = l_ref[pl.ds(pl.multiple_of(block * 2 * TILES, 2 * TILES), 2 * TILES), :]
    out = dot(left, w_ref[pairs * block])
    for k in range(1, pairs):
        out = jnp.where(of_pair == k, dot(left, w_ref[pairs * block + k]), out)
    finish(pl.multiple_of(block * TILES, TILES), out[:TILES] + out[TILES:])


def run_tiles(w_ref, l_ref, most, finish):
    blocks = w_ref.shape[0] // (TILES // 2)
    unroll = next(n for n in (most, 6, 4, 3, 2, 1) if blocks % n == 0)

    def body(step, carry):
        for inner in range(unroll):
            one_block(w_ref, l_ref, step * unroll + inner, finish)
        return carry

    lax.fori_loop(0, blocks // unroll, body, 0)


def forward_left(vec, gf_ref, l_ref):
    picked = gather(gf_ref, vec)
    first = lax.broadcasted_iota(jnp.int32, picked.shape, 0) % 2 == 0
    zero = jnp.zeros_like(picked)
    l_ref[:, :LANES] = jnp.where(first, picked, zero).astype(BF16)
    l_ref[:, LANES:] = jnp.where(first, zero, picked).astype(BF16)


def forward_finish(out_ref):
    def finish(at, out):
        out_ref[pl.ds(at, TILES), :] = out[:, :LANES] + out[:, LANES:]

    return finish


def forward_parts(vec, gf_ref, wt_ref, out_ref, l_ref):
    forward_left(vec, gf_ref, l_ref)
    run_tiles(wt_ref, l_ref, UNROLL, forward_finish(out_ref))


def backward_sum(vec, gb_ref, sb_ref, w_ref, l_ref, rows_ref):
    picked = gather(gb_ref, vec).astype(BF16)
    l_ref[:, :LANES] = picked
    l_ref[:, LANES:] = picked
    first = lax.broadcasted_iota(jnp.int32, (TILES, LANES), 0) % 2 == 0

    def finish(at, out):
        rows_ref[pl.ds(at, TILES), :] = jnp.where(first, out[:, :LANES], out[:, LANES:])

    run_tiles(w_ref, l_ref, UNROLL, finish)
    return scatter(sb_ref[...], rows_ref[...])


def gathered_rows(part_refs, s_ref):
    count = s_ref.shape[2]
    return tree(scatter(s_ref[j], ref[:count, :]) for j, ref in enumerate(part_refs))


def put_halves(refs, total, extra):
    half = total.shape[0] // 2
    for ref, part in zip(refs, (total[:half], total[half:])):
        ref[:half, :] = part
        ref[half:, :] = extra


def select_columns(ref, rows):
    size, count = ref.shape
    for row in range(pl.cdiv(count, LANES)):
        width = min(LANES, count - row * LANES)
        hit = lax.broadcasted_iota(jnp.int32, (size, width), 0) == rows[row : row + 1, :width].astype(jnp.int32)
        ref[:, row * LANES : row * LANES + width] = jnp.where(hit, 1.0, 0.0).astype(BF16)


def select_rows(ref, rows):
    count, size = ref.shape
    across = rows.T.astype(jnp.int32)
    for row in range(pl.cdiv(count, LANES)):
        width = min(LANES, count - row * LANES)
        hit = lax.broadcasted_iota(jnp.int32, (width, size), 1) == across[:width, row : row + 1]
        ref[row * LANES : row * LANES + width, :] = jnp.where(hit, 1.0, 0.0).astype(BF16)


def tile_copies(chunk, refs, held_ref, sems):
    copies, at = [], 0
    for ref in refs:
        for start in range(0, ref.shape[0], chunk):
            copies.append(
                pltpu.make_async_copy(
                    ref.at[pl.ds(start, chunk)], held_ref.at[pl.ds(at, chunk)], sems.at[len(copies)]
                )
            )
            at += chunk
    return copies


def wait_chunk(step, chunk, copies, a_ref, held_ref, sems):
    for later in range(IN_FLIGHT, len(copies)):
        pl.when(step + IN_FLIGHT == later)(copies[later].start)
    at = pl.multiple_of(step * chunk, chunk)
    pltpu.make_async_copy(a_ref.at[pl.ds(0, chunk)], held_ref.at[pl.ds(at, chunk)], sems.at[step]).wait()


def odd_core():
    return lax.axis_index("row") % 2 == 1


def split_kernel(chunk, a_ref, g_ref, w_ref, sq_ref, held_ref, sems):
    copies = tile_copies(chunk, (a_ref, g_ref), held_ref, sems)
    for copy in copies:
        copy.start()

    def body(step, carry):
        wait_chunk(step, chunk, (), a_ref, held_ref, sems)
        for t in range(chunk):
            tile = held_ref[step * chunk + t]
            pair, at = (step * chunk + t) // 2, (t % 2) * LANES
            high, low = split2(tile)
            w_ref[pair, :LANES, at : at + LANES] = high
            w_ref[pair, LANES:, at : at + LANES] = low
            sq_ref[pl.ds(step * chunk + t, 1), :] = row_sum(tile * tile)
        return carry

    lax.fori_loop(0, len(copies), body, 0)


def turned_places(odd, places, xcount):
    half = xcount // 2
    moved = jnp.where(places >= half, places - half, places + half)
    return jnp.where(odd, moved, places)


def joined(at_ref, a_ref, f_ref, base=0):
    acount, fcount = a_ref.shape[1], f_ref.shape[1]
    at_ref[...] = jnp.zeros_like(at_ref)
    at_ref[0:1, :acount] = a_ref[...].astype(F32)
    at_ref[1:2, :fcount] = (f_ref[...] + base).astype(F32)
    a, f = at_ref[0:1, :], at_ref[1:2, :]
    moved = pltpu.roll(jnp.broadcast_to(f, (8, LANES)), acount % LANES, 1)[0:1]
    lane = lax.broadcasted_iota(jnp.int32, (1, LANES), 1)
    return [jnp.where(lane < acount, a, moved), moved]


def first_forward_kernel(chunk, ycount, rho_ref, *refs):
    (a_ref, g_ref), small_refs, refs = refs[:2], refs[2:7], refs[7:]
    (wt_ref, out_ref, v_ref, gf_ref, l_ref, at_ref), refs = refs[:6], refs[6:]
    small_held, (small_sems, held_ref, sems) = refs[:5], refs[5:]
    fetched = [pltpu.make_async_copy(a, b, small_sems.at[i]) for i, (a, b) in enumerate(zip(small_refs, small_held))]
    copies = tile_copies(chunk, (a_ref, g_ref), held_ref, sems)
    for copy in fetched + copies[:1]:
        copy.start()
    odd = odd_core()
    for copy in fetched:
        copy.wait()
    for copy in copies[1:IN_FLIGHT]:
        copy.start()
    v_in_ref, arow_ref, acol_ref, frow_ref, fcol_ref = small_held
    count = 2 * wt_ref.shape[0]
    v = turn(odd, v_in_ref[...])
    v_ref[...] = v
    zero = [jnp.zeros((1, LANES), F32)] * 2
    yrows = joined(at_ref, arow_ref, frow_ref, ycount) + zero
    xrows = joined(at_ref, acol_ref, fcol_ref) + zero
    out_ref[count:, :] = jnp.concatenate(yrows + xrows, axis=0)
    places = jnp.concatenate(xrows + yrows, axis=0)
    select_rows(gf_ref, turned_places(odd, places, v.shape[0]))
    forward_left(v, gf_ref, l_ref)
    finish = forward_finish(out_ref)

    def split(step):
        wait_chunk(step, chunk, copies, a_ref, held_ref, sems)
        for t in range(chunk):
            pair, at = (step * chunk + t) // 2, (t % 2) * LANES
            high, low = split2(held_ref[step * chunk + t].T)
            wt_ref[pair, at : at + LANES, :LANES] = high
            wt_ref[pair, at : at + LANES, LANES:] = low

    def body(step, carry):
        split(step)
        return carry

    lax.fori_loop(0, len(copies), body, 0)
    run_tiles(wt_ref, l_ref, UNROLL, finish)


def first_backward_kernel(n_col, ycount, acount, *refs):
    rho_ref, *refs = refs
    part_refs, refs = refs[:n_col], refs[n_col:]
    (w_ref, sq_ref, slack_ref, dual_ref), refs = refs[:4], refs[4:]
    mine_ref, theirs_ref, y_ref, s_ref, gb_ref, sb_ref, l_ref, rows_ref = refs
    rho, odd = rho_ref[0], odd_core()
    count = s_ref.shape[2]
    for j, ref in enumerate(part_refs):
        select_columns(s_ref.at[j], ref[count:, :])
    places = part_refs[0][count:, :]
    select_rows(gb_ref, places)
    select_columns(sb_ref, turned_places(odd, places[4:], sb_ref.shape[0]))
    full = gathered_rows(part_refs, s_ref)
    y_ref[...] = full
    top = rho * slack_ref[...] - dual_ref[...] - rho * full[:ycount]
    vec = jnp.concatenate([top, -full[ycount:]], axis=0)
    total = backward_sum(vec, gb_ref, sb_ref, w_ref, l_ref, rows_ref)
    squares = sq_ref[...]
    is_a = lax.broadcasted_iota(jnp.int32, squares.shape, 0) < acount
    parts = split3(jnp.where(is_a, rho * squares, squares))
    squares = sum(dot(sb_ref[...], part) for part in parts)
    half = total.shape[0] // 2
    mine_ref[:half, :] = total[:half]
    mine_ref[half:, :] = squares[:half]
    theirs_ref[:half, :] = total[half:]
    theirs_ref[half:, :] = squares[half:]


def finish_forward(u, p, resid, shifted, out_ref, gf_ref, w_ref, l_ref):
    count = 2 * w_ref.shape[0]
    weighted = shifted * u
    rows = [half_sum(resid * u), half_sum(weighted * u)]
    if p is not None:
        rows.append(half_sum(weighted * p))
    out_ref[count:, :] = pad_rows(rows)
    forward_parts(u, gf_ref, w_ref, out_ref, l_ref)


def second_forward_kernel(mine_ref, theirs_ref, v_ref, d_in_ref, c_in_ref, gf_ref, w_ref, *refs):
    r_ref, u_ref, pre_ref, d_ref, c_ref, out_ref, l_ref = refs
    odd = odd_core()
    half = v_ref.shape[0] // 2
    total = jnp.concatenate([mine_ref[:half, :], theirs_ref[:half, :]], axis=0)
    squares = jnp.concatenate([mine_ref[half:, :], theirs_ref[half:, :]], axis=0)
    v, d, c = v_ref[...], turn(odd, d_in_ref[...]), turn(odd, c_in_ref[...])
    d_ref[...] = d
    c_ref[...] = c
    resid = total - c - d * v
    shifted = d + SIGMA
    pre = shifted + squares
    u = resid / pre
    r_ref[...] = resid
    u_ref[...] = u
    pre_ref[...] = pre
    finish_forward(u, None, resid, shifted, out_ref, gf_ref, w_ref, l_ref)


def step_scalars(first, part_refs, sc_old_ref, count):
    totals = jnp.sum(tree(ref[count:, :] for ref in part_refs), axis=1, keepdims=True)
    gamma, one, two = totals[0:1], totals[1:2], totals[2:3]
    if first:
        return gamma, jnp.zeros_like(gamma), one
    old = sc_old_ref[...]
    beta = gamma / old[0:1, 0:1]
    return gamma, beta, one + beta * (2.0 * two + beta * old[2:3, 0:1])


def wide(x):
    return jnp.broadcast_to(x, (1, LANES))


def backward_kernel(n_col, ycount, first, last, *refs):
    rho_ref, *refs = refs
    part_refs, refs = refs[:n_col], refs[n_col:]
    s_ref, refs = refs[0], refs[1:]
    sc_old_ref = None
    if not first:
        (yp_old_ref, yv_old_ref, sc_old_ref, alpha_ref), refs = refs[:4], refs[4:]
    else:
        (yv_old_ref,), refs = refs[:1], refs[1:]
    if not last:
        (gb_ref, sb_ref, w_ref), refs = refs[:3], refs[3:]
    if last:
        z_ref, *refs = refs
    else:
        mine_ref, theirs_ref, *refs = refs
    yp_ref, yv_ref, sc_ref, *scratch = refs
    rho = rho_ref[0]
    full = gathered_rows(part_refs, s_ref)
    gamma, beta, pdp = step_scalars(first, part_refs, sc_old_ref, s_ref.shape[2])
    sc_ref[...] = pad_rows([wide(gamma), wide(beta), wide(pdp)])
    if first:
        yp = full
        yv_ref[...] = yv_old_ref[...]
    else:
        yp_old = yp_old_ref[...]
        yp = full + beta * yp_old
        yv_ref[...] = yv_old_ref[...] + alpha_ref[0:1, 0:1] * yp_old
    yp_ref[...] = yp
    scaled = jnp.concatenate([rho * yp[:ycount], yp[ycount:]], axis=0)
    norm = pad_rows([row_sum(scaled * yp)])
    if last:
        z_ref[...] = norm
    else:
        put_halves((mine_ref, theirs_ref), backward_sum(scaled, gb_ref, sb_ref, w_ref, *scratch), norm)


def step_alpha(extra, sc_ref):
    norm = jnp.sum(extra[0:1], axis=1, keepdims=True)
    return sc_ref[0:1, 0:1] / (sc_ref[2:3, 0:1] + norm)


def forward_kernel(first, *refs):
    (mine_ref, theirs_ref), refs = refs[:2], refs[2:]
    if not first:
        p_old_ref, refs = refs[0], refs[1:]
    (u_old_ref, v_old_ref, r_old_ref, d_ref, pre_ref, sc_ref, gf_ref, w_ref), refs = refs[:8], refs[8:]
    p_ref, v_ref, r_ref, u_ref, alpha_ref, out_ref, *scratch = refs
    half = d_ref.shape[0] // 2
    total = jnp.concatenate([mine_ref[:half, :], theirs_ref[:half, :]], axis=0)
    alpha = step_alpha(mine_ref[half:, :], sc_ref)
    p = u_old_ref[...]
    if not first:
        p = p + sc_ref[1:2, 0:1] * p_old_ref[...]
    shifted = d_ref[...] + SIGMA
    resid = r_old_ref[...] - alpha * (shifted * p + total)
    u = resid / pre_ref[...]
    p_ref[...] = p
    v_ref[...] = v_old_ref[...] + alpha * p
    r_ref[...] = resid
    u_ref[...] = u
    alpha_ref[...] = jnp.broadcast_to(alpha, (8, LANES))
    finish_forward(u, p, resid, shifted, out_ref, gf_ref, w_ref, *scratch)


def final_kernel(ycount, *refs):
    rho_ref, t_ref, *refs = refs
    (u_ref, p_old_ref, v_ref, start_ref, sc_ref, yp_ref, yv_ref, y0_ref), refs = refs[:8], refs[8:]
    (slack_ref, dual_ref, lower_ref, upper_ref, gb_ref, sb_ref, w_ref), refs = refs[:7], refs[7:]
    primal_out, half_out, slack_out, dual_out, mine_ref, theirs_ref, *scratch = refs
    rho = rho_ref[0]
    alpha = step_alpha(t_ref[...], sc_ref)
    p = u_ref[...] + sc_ref[1:2, 0:1] * p_old_ref[...]
    v = v_ref[...] + alpha * p
    primal = RELAX * v + (1.0 - RELAX) * start_ref[...]
    primal_out[...] = turn(odd_core(), primal)
    half_out[...] = primal[: primal.shape[0] // 2]
    image = yv_ref[...] + alpha * yp_ref[...]
    image_next = RELAX * image + (1.0 - RELAX) * y0_ref[...]
    dual = dual_ref[...]
    relaxed = RELAX * image[:ycount] + (1.0 - RELAX) * slack_ref[...]
    slack_next = jnp.minimum(jnp.maximum(relaxed + dual / rho, lower_ref[...]), upper_ref[...])
    dual_next = dual + rho * (relaxed - slack_next)
    slack_out[...] = slack_next
    dual_out[...] = dual_next
    worst = jnp.max(jnp.abs(image_next[:ycount] - slack_next), axis=0, keepdims=True)
    vec = jnp.concatenate([dual_next, image_next[ycount:]], axis=0)
    total = backward_sum(vec, gb_ref, sb_ref, w_ref, *scratch)
    put_halves((mine_ref, theirs_ref), total, jnp.broadcast_to(worst, (8, LANES)))


def residual_kernel(z_ref, primal_ref, d_ref, c_ref, out_ref):
    half = d_ref.shape[0] // 2
    dvec = d_ref[:half, :] * primal_ref[...] + z_ref[:half, :] + c_ref[:half, :]
    worst = jnp.max(jnp.abs(dvec), axis=0, keepdims=True)
    out_ref[...] = jnp.concatenate([z_ref[half : half + 4, :], jnp.broadcast_to(worst, (4, LANES))], axis=0)


VMEM_SPEC = pl.BlockSpec(memory_space=pltpu.VMEM)
SMEM_SPEC = pl.BlockSpec(memory_space=pltpu.SMEM)
HBM_SPEC = pl.BlockSpec(memory_space=pltpu.HBM)


def call(kernel, name, outs, args, scratch=(), scalars=0, streamed=0, cost=None):
    kinds = [SMEM_SPEC] * scalars + [HBM_SPEC] * streamed
    specs = kinds + [VMEM_SPEC] * (len(args) - len(kinds))
    args = [
        pltpu.with_memory_space_constraint(x, pltpu.HBM) if scalars <= i < scalars + streamed else x
        for i, x in enumerate(args)
    ]
    shapes = tuple(s if isinstance(s, jax.ShapeDtypeStruct) else jax.ShapeDtypeStruct(s, F32) for s in outs)
    return pl.pallas_call(
        kernel,
        out_shape=shapes,
        in_specs=specs,
        out_specs=tuple(VMEM_SPEC for _ in outs),
        scratch_shapes=list(scratch),
        compiler_params=pltpu.CompilerParams(vmem_limit_bytes=VMEM_LIMIT),
        cost_estimate=cost,
        name=name,
    )(*args)


def swap(x, axis, size, distance):
    return lax.ppermute(x, axis, [(i, i ^ distance) for i in range(size)])


def exchange(x, axis, size, distances):
    return [x] + [swap(x, axis, size, m) for m in distances]


def local(n_row, n_col, *args):
    (
        constraint_tiles,
        constraint_rows,
        constraint_cols,
        factor_tiles,
        factor_rows,
        factor_cols,
        diag_cost,
        linear_cost,
        lower_bound,
        upper_bound,
        primal_start,
        slack_start,
        dual_start,
        penalty,
    ) = args
    width = constraint_tiles.shape[2]
    ctiles = constraint_tiles.reshape(-1, width, width)
    ftiles = factor_tiles.reshape(-1, width, width)
    acount, fcount = ctiles.shape[0], ftiles.shape[0]
    count = acount + fcount
    pairs = count // 2
    xcount = primal_start.shape[0]
    ycount = slack_start.shape[0]
    full = ycount + YG
    half = xcount // 2

    def over_col(x):
        return exchange(x, "col", n_col, range(1, n_col))

    def over_plane(chip, op=jnp.add):
        return tree(exchange(chip, "row", n_row, range(2, n_row, 2)), op)

    def other_core(x):
        return swap(x, "row", n_row, 1)

    def over_row(mine, theirs):
        summed = over_plane(mine + other_core(theirs))
        return summed, other_core(summed)

    rho = penalty.reshape(1)
    chunk = next(n for n in (24, 16, 8) if acount % n == 0 and fcount % n == 0)
    assert acount <= width and fcount <= width
    matrices = jax.ShapeDtypeStruct((pairs, 2 * width, 2 * width), BF16)
    held = [
        pltpu.VMEM((count, width, width), F32),
        pltpu.SemaphoreType.DMA((count // chunk,)),
    ]

    left = pltpu.VMEM((2 * count, 2 * width), BF16)
    rows = pltpu.VMEM((count, width), F32)
    xs, ys, small = (xcount, width), (full, width), (8, width)
    sent, summed = (count + 8, width), (half + 8, width)
    bits = functools.partial(jax.ShapeDtypeStruct, dtype=BF16)

    turned, parts, start, gf = call(
        functools.partial(first_forward_kernel, chunk, ycount),
        "first_forward",
        [matrices, sent, xs, bits((count, xcount))],
        (rho, ctiles, ftiles, primal_start)
        + tuple(x.reshape(1, -1) for x in (constraint_rows, constraint_cols, factor_rows, factor_cols)),
        [left, pltpu.VMEM((8, width), F32), pltpu.VMEM(xs, F32)]
        + [pltpu.VMEM((1, n), jnp.int32) for n in (acount, acount, fcount, fcount)]
        + [pltpu.SemaphoreType.DMA((5,)), *held],
        scalars=1,
        streamed=7,
    )
    parts, ctiles, ftiles = lax.optimization_barrier((parts, ctiles, ftiles))
    all_parts = over_col(parts)
    tiles, squares = call(
        functools.partial(split_kernel, chunk),
        "split",
        [matrices, (count, width)],
        (ctiles, ftiles),
        held,
        streamed=2,
        cost=pl.CostEstimate(
            flops=8 * count * width * width, bytes_accessed=4 * count * width * width, transcendentals=0
        ),
    )
    mine, theirs, y0, s_all, gb, sb = call(
        functools.partial(first_backward_kernel, n_col, ycount, acount),
        "first_backward",
        [xs, xs, ys, bits((n_col, full, count)), bits((count, full)), bits((xcount, count))],
        (rho, *all_parts, tiles, squares, slack_start, dual_start),
        [left, rows],
        scalars=1,
    )
    resid, u, precond, diag, linear, parts = call(
        second_forward_kernel,
        "second_forward",
        [xs, xs, xs, xs, xs, sent],
        (*over_row(mine, theirs), start, diag_cost, linear_cost, gf, turned),
        [left],
    )
    v, yv = start, y0
    p = yp = sc = alpha = None
    for step in range(CG):
        first, last = step == 0, step + 1 == CG
        state = (yv,) if first else (yp, yv, sc, alpha)
        mats = () if last else (gb, sb, tiles)
        *z, yp, yv, sc = call(
            functools.partial(backward_kernel, n_col, ycount, first, last),
            "last_norm" if last else "backward",
            ([small] if last else [summed, summed]) + [ys, ys, small],
            (rho, *over_col(parts), s_all, *state, *mats),
            [] if last else [left, rows],
            scalars=1,
        )
        if last:
            break
        p, v, resid, u, alpha, parts = call(
            functools.partial(forward_kernel, first),
            "forward",
            [xs, xs, xs, xs, small, sent],
            (*over_row(*z), *(() if first else (p,)), u, v, resid, diag, precond, sc, gf, turned),
            [left],
        )
    norm = over_plane(z[0] + other_core(z[0]))
    primal_next, primal_half, slack_next, dual_next, mine, theirs = call(
        functools.partial(final_kernel, ycount),
        "final",
        [xs, (half, width), (ycount, width), (ycount, width), summed, summed],
        (rho, norm, u, p, v, start, sc, yp, yv, y0)
        + (slack_start, dual_start, lower_bound, upper_bound, gb, sb, tiles),
        [left, rows],
        scalars=1,
    )

    def join(a, b):
        is_sum = lax.broadcasted_iota(jnp.int32, a.shape, 0) < half
        return jnp.where(is_sum, a + b, jnp.maximum(a, b))

    z = over_plane(join(mine, other_core(theirs)), join)
    (worst,) = call(residual_kernel, "residuals", [small], (z, primal_half, diag, linear))
    worst = jnp.maximum(worst, other_core(worst))
    worst = tree(over_col(worst), jnp.maximum)
    return (primal_next, slack_next, dual_next, jnp.max(worst[:4]), jnp.max(worst[4:]))


def solution(mesh):
    placed = (
        P("row", "col", None, None),
        P("row", "col"),
        P("row", "col"),
        P("row", "col", None, None),
        P("row", "col"),
        P("row", "col"),
        P("col", None),
        P("col", None),
        P("row", None),
        P("row", None),
        P("col", None),
        P("row", None),
        P("row", None),
        P(),
    )
    return jax.shard_map(
        functools.partial(local, mesh.shape["row"], mesh.shape["col"]),
        mesh=mesh,
        in_specs=placed,
        out_specs=(P("col", None), P("row", None), P("row", None), P(), P()),
        check_vma=False,
    )
```
